32 devices in a mesh: grid: 16 (over z, x, core), band: 2 (over y).
Axes of the slice: x: 2, y: 2, z: 4, core: 2. Of those that a mesh axis runs over, the one named last changes fastest.
Arguments:
- left_bands: float32 [2, 8, 128, 128, 128], P(None, 'band', 'grid'), may hold values from -6 to 6
- right_bands: float32 [2, 4, 128, 128, 128], P(None, 'band', 'grid'), may hold values from -6 to 6
- sphere_index: int32 [16384], replicated, may hold values from 0 to 2097151, as said below
- right_order: int32 [4], replicated, may hold values from 0 to 3, each once
Outputs:
- pair_density: float32 [2, 8, 4, 16384], P(None, 'band', None, 'grid')
The draws below stay inside these ranges and needn't reach their ends.
Inputs may be any that keep to these rules, and one draw needn't show every extreme that they name: `sphere_index`: flat index (kz * 128 + ky) * 128 + kx; an index may repeat. In each aligned block of 1024 entries, at most 64 entries share one value of ky // 8, and some value is shared by exactly 64. `right_order`: each second band once.
All inputs are finite; a program needn't handle non-finite values.
Results may differ from the reference program's by a relative error of at most 0.00008.
Values sent between devices are 32-bit elements; how exact they have to be, the bound alone decides.
No kernel may reach another device: no remote copies, remote signals or barrier semaphores. Data moves between devices by JAX's collectives and lax.ppermute only.
A program may use at most 256 MiB of HBM per device.

```python
import jax
import jax.numpy as jnp
from jax import lax

NG = 128
NX = 128
NGV = 16384
NL = 8
NR = 4
ZS = 8


def draw_sphere_index(key, part):
    devices = NG // ZS
    per_block = NGV // devices
    key_shift = jax.random.fold_in(key, 11)
    key_perm = jax.random.fold_in(key, 12)
    key_row = jax.random.fold_in(key, 13)
    key_plane = jax.random.fold_in(key, 14)
    key_column = jax.random.fold_in(key, 15)
    shifts = jax.random.randint(key_shift, (devices, 1), 0, devices)
    position = jnp.arange(per_block, dtype=jnp.int32)[None, :]
    source = (position + shifts) % devices
    block_keys = jax.random.split(key_perm, devices)
    orders = jax.vmap(lambda k: jax.random.permutation(k, per_block))(block_keys)
    source = jnp.take_along_axis(source, orders.astype(jnp.int32), axis=1).reshape(-1)
    wave_y = source * ZS + jax.random.randint(key_row, (NGV,), 0, ZS)
    wave_z = jax.random.randint(key_plane, (NGV,), 0, NG)
    wave_x = jax.random.randint(key_column, (NGV,), 0, NX)
    return ((wave_z * NG + wave_y) * NX + wave_x).astype(jnp.int32)


def levels(stream_key, shape, shards, low, top_value):
    def one(dim, parts):
        draws = jax.random.uniform(jax.random.fold_in(jax.random.fold_in(stream_key, 6), dim), (parts,), jnp.float32, low / len(shards), top_value / len(shards))
        return jnp.repeat(jnp.exp(draws), shape[dim] // parts).reshape((-1,) + (1,) * (len(shape) - dim - 1))

    factor_of = one(*shards[0])
    for cut in shards[1:]:
        factor_of = factor_of * one(*cut)
    return factor_of


def normal_values(stream_key, dims, scale, reach, cuts=(), kind=jnp.bfloat16):
    array = jax.random.normal(stream_key, dims, jnp.float32) * scale
    if len(cuts) > 0:
        array = levels(stream_key, dims, cuts, -0.22, 0.18) * array
    return jnp.clip(array, min=-reach, max=reach).astype(kind)


def setup_inputs(seed: int = 0) -> dict:
    key_list = jax.random.split(jax.random.key(seed), 5)
    return {
        "left_bands": normal_values(key_list[0], (2, NL, NG, NG, NX), 1.0, 6.0, ((1, 2), (2, 16)), jnp.float32),
        "right_bands": normal_values(key_list[1], (2, NR, NG, NG, NX), 1.0, 6.0, ((1, 2), (2, 16)), jnp.float32),
        "sphere_index": draw_sphere_index(jax.random.fold_in(key_list[4], 71), 0),
        "right_order": jax.random.permutation(key_list[3], NR).astype(jnp.int32),
    }


def reference(left_bands, right_bands, sphere_index, right_order):
    factor = 1.0 / (NG * NG * NX) ** 0.5

    def one_left(left_field):
        def one_right(column):
            right_field = lax.dynamic_index_in_dim(right_bands, column, 1, keepdims=False)
            real_part = left_field[0] * right_field[0] + left_field[1] * right_field[1]
            imag_part = left_field[0] * right_field[1] - left_field[1] * right_field[0]
            spectrum = jnp.fft.fftn(real_part + 1j * imag_part)
            picked = spectrum.reshape(-1)[sphere_index]
            return jnp.stack([jnp.real(picked), jnp.imag(picked)]).astype(jnp.float32) * factor

        return lax.map(one_right, right_order)

    result = lax.map(one_left, jnp.moveaxis(left_bands, 1, 0))
    return jnp.transpose(result, (2, 0, 1, 3))
```

```python
from functools import partial
import math

import jax
import jax.numpy as jnp
import numpy as np
from jax import lax
from jax.experimental import pallas as pl
from jax.experimental.pallas import tpu as pltpu
from jax.sharding import PartitionSpec as P

F32 = jnp.float32
BF16 = jnp.bfloat16
LANES = 128
SUB = 8


def swapped(block, axis, apart):
    count = lax.axis_size(axis)
    route = []
    for low in range(count):
        high = low | 1 << apart
        if high != low and high < count:
            route += [(low, high), (high, low)]
    return lax.ppermute(block, axis, route)


def dft_parts(length):
    counter = np.arange(length)
    angles = (counter[:, None] * counter[None, :] % length) * (2.0 * math.pi / length)
    return np.cos(angles), np.sin(angles)


def two_terms(table):
    table = jnp.asarray(table, F32)
    high = table.astype(BF16)
    return jnp.stack([high, (table - high.astype(F32)).astype(BF16)])


def rows_table(length):
    cosine, sine = dft_parts(length)
    return np.block([[cosine, sine], [-sine, cosine]]).astype(np.float32)


def lanes_table(length):
    cosine, sine = dft_parts(length)
    return np.block([[cosine, -sine], [sine, cosine]]).astype(np.float32)


def split(value):
    high = value.astype(BF16)
    return high, (value - high.astype(F32)).astype(BF16)


def dot(a, b):
    return jnp.dot(a, b, preferred_element_type=F32)


def taken(value, lanes):
    return jnp.take_along_axis(value, lanes, axis=1, mode="promise_in_bounds")


def chunk_kernel(
    plan, left_ref, right_ref, table_y_ref, table_x_ref, picks_ref, turns_ref, *rest
):
    if plan["add"]:
        before_ref, out_ref, h_real, h_imag, f_even, f_odd = rest
    else:
        out_ref, h_real, h_imag, f_even, f_odd = rest
    lefts, rights, planes = plan["lefts"], plan["rights"], plan["planes"]
    pairs = lefts * rights
    halves, tiles, stride = plan["halves"], plan["tiles"], plan["stride"]
    length, groups, rows, chunks = plan["length"], plan["groups"], plan["rows"], plan["chunks"]
    wide = tiles * SUB

    def transform_rows(z, _):
        if halves == 2:
            slot = (z % tiles) * SUB + (z // tiles) * pairs
        else:
            slot = z * SUB
        for first in range(0, pairs, 2):
            fields = []
            for pair in (first, first + 1):
                m, n = pair // lefts, pair % lefts
                lr, li = left_ref[0, n, z], left_ref[1, n, z]
                rr, ri = right_ref[0, m, z], right_ref[1, m, z]
                fields.append(jnp.concatenate([lr * rr + li * ri, lr * ri - li * rr], axis=0))
            high, low = split(jnp.concatenate(fields, axis=1))
            moved = dot(table_y_ref[0], high) + dot(table_y_ref[1], high) + dot(table_y_ref[0], low)
            for k in range(2):
                spot = pl.ds(slot + first + k, length, stride=stride)
                lanes = slice(k * LANES, (k + 1) * LANES)
                h_real[spot, :] = moved[:length, lanes]
                h_imag[spot, :] = moved[length:, lanes]
        return 0

    lax.fori_loop(0, planes, transform_rows, 0)

    def transform_lanes(group, f_ref):
        for y in range(rows):
            spot = pl.ds((group * rows + y) * stride, wide)
            high, low = split(jnp.concatenate([h_real[spot, :], h_imag[spot, :]], axis=1))
            f_ref[y] = (
                dot(high, table_x_ref[0]) + dot(low, table_x_ref[0]) + dot(high, table_x_ref[1])
            )

    upper = lax.broadcasted_iota(jnp.int32, (SUB, LANES), 0) >= SUB // 2
    late = lax.broadcasted_iota(jnp.int32, (SUB, LANES), 1) >= LANES // 2

    def picked(group, chunk, f_ref):
        at = group * chunks + chunk

        def wide_row(ref, k):
            return jnp.broadcast_to(ref[k, pl.ds(at, 1), :], (SUB, LANES))

        lanes = wide_row(picks_ref, 0)
        y_of = wide_row(picks_ref, 1)
        same = [y_of == y for y in range(rows)]
        turn_r, turn_i = wide_row(turns_ref, 0), wide_row(turns_ref, 1)
        base_r, base_i = wide_row(turns_ref, 2), wide_row(turns_ref, 3)
        if halves == 2:
            base_r = jnp.where(upper, wide_row(turns_ref, 4), base_r)
            base_i = jnp.where(upper, wide_row(turns_ref, 5), base_i)

        def value(tile, part):
            box = (slice(tile * SUB, (tile + 1) * SUB), slice(part * LANES, (part + 1) * LANES))
            best = taken(f_ref[(0,) + box], lanes)
            for y in range(1, rows):
                best = jnp.where(same[y], taken(f_ref[(y,) + box], lanes), best)
            return best

        real, imag = value(tiles - 1, 0), value(tiles - 1, 1)
        for tile in reversed(range(tiles - 1)):
            real, imag = (
                real * turn_r - imag * turn_i + value(tile, 0),
                real * turn_i + imag * turn_r + value(tile, 1),
            )
        real, imag = real * base_r - imag * base_i, real * base_i + imag * base_r
        if pairs == SUB:
            return [real, imag]
        if halves == 2:
            real = real + pltpu.roll(real, SUB // 2, 0)
            imag = imag + pltpu.roll(imag, SUB // 2, 0)
        else:
            imag = pltpu.roll(imag, SUB // 2, 0)
        return [jnp.where(upper, imag, real)]

    def put(spot, value):
        if plan["add"]:
            value = value + before_ref[spot]
        out_ref[spot] = value

    if plan["woven"]:
        transform_lanes(0, f_even)

        def couple(a, _):
            even = 2 * a
            firsts = []
            transform_lanes(even + 1, f_odd)
            for chunk in range(chunks):
                firsts.append(picked(even, chunk, f_even))
            transform_lanes(jnp.minimum(even + 2, groups - 1), f_even)
            place = pl.ds(pl.multiple_of(a * LANES, LANES), LANES)
            for chunk in range(chunks):
                seconds = picked(even + 1, chunk, f_odd)
                for part, (one, two) in enumerate(zip(firsts[chunk], seconds)):
                    put(
                        (2 * chunk, part, slice(None), place),
                        jnp.where(late, pltpu.roll(two, LANES // 2, 1), one),
                    )
                    put(
                        (2 * chunk + 1, part, slice(None), place),
                        jnp.where(late, two, pltpu.roll(one, LANES // 2, 1)),
                    )
            return 0

        lax.fori_loop(0, groups // 2, couple, 0)
    else:

        def single(group, _):
            transform_lanes(group, f_even)
            for chunk in range(chunks):
                for part, value in enumerate(picked(group, chunk, f_even)):
                    put((group * chunks + chunk, part), value)
            return 0

        lax.fori_loop(0, groups, single, 0)


def chunk_sums(left, right, tables, picks, turns, before, sizes):
    lefts, rights = left.shape[1], right.shape[1]
    planes, length = left.shape[2], left.shape[3]
    groups, slots = sizes
    pairs = lefts * rights
    halves = 2 if pairs < SUB and planes % 2 == 0 else 1
    tiles = planes // halves
    wide = tiles * SUB
    stride = wide if tiles % 2 else wide + SUB
    parts = 2 * pairs // SUB
    chunks = groups * slots // LANES
    woven = 2 * slots == LANES and groups % 2 == 0
    plan = dict(
        lefts=lefts, rights=rights, planes=planes, halves=halves, tiles=tiles, stride=stride,
        length=length, groups=groups, rows=length // groups, chunks=chunks, woven=woven,
        add=before is not None,
    )
    if woven:
        shape = (groups, parts, SUB, groups * slots)
    else:
        shape = (groups * chunks, parts, SUB, LANES)
    operands = [left, right, *tables, picks, turns]
    if before is not None:
        operands.append(before)
    field = pltpu.VMEM((length * stride, LANES), F32)
    group = pltpu.VMEM((length // groups, wide, 2 * LANES), F32)
    flops = 2 * 3 * 2 * pairs * planes * length * (2 * length) * (2 * length)
    return pl.pallas_call(
        partial(chunk_kernel, plan),
        out_shape=jax.ShapeDtypeStruct(shape, F32),
        scratch_shapes=[field, field, group, group],
        compiler_params=pltpu.CompilerParams(vmem_limit_bytes=60000 * 1024),
        cost_estimate=pl.CostEstimate(flops=flops, bytes_accessed=4 * left.size, transcendentals=0),
    )(*operands)


def to_owner(sums, sizes):
    groups, slots = sizes
    if sums.shape[0] == groups and sums.shape[-1] == groups * slots:
        return sums
    parts = sums.shape[1]
    shaped = sums.reshape(groups, -1, parts, SUB, LANES)
    shaped = jnp.moveaxis(shaped, 1, 3).reshape(groups, parts, SUB, groups, slots)
    return jnp.transpose(shaped, (3, 1, 2, 0, 4)).reshape(groups, parts, SUB, groups * slots)


def finish_kernel(scale, count, own_rights, order_ref, place_ref, own_ref, *rest):
    others, out_ref, hold_ref = rest[:count], rest[count], rest[count + 1]
    length = out_ref.shape[-1]
    lefts = out_ref.shape[1]
    half = SUB // 2

    def total(ref, part):
        value = ref[0, part]
        for source in range(1, ref.shape[0]):
            value = value + ref[source, part]
        return value * scale

    blocks = [[total(own_ref, part) for part in range(own_ref.shape[1])]]
    if len(blocks[0]) == 2:
        real, imag = blocks[0]
        for m in range(own_rights):
            rows = slice(m * lefts, (m + 1) * lefts)
            hold_ref[m] = jnp.concatenate([real[rows], imag[rows]], axis=0)
    for k, ref in enumerate(others):
        hold_ref[own_rights + k] = total(ref, 0)
    pieces = length // LANES
    for j in range(out_ref.shape[2]):
        block = hold_ref[order_ref[j]]
        for piece in range(pieces):
            lanes = slice(piece * LANES, (piece + 1) * LANES)
            place = jnp.broadcast_to(place_ref[:, lanes], (SUB, LANES))
            inner = place % LANES
            outer = place // LANES
            best = taken(block[:, :LANES], inner)
            for source in range(1, pieces):
                more = taken(block[:, source * LANES : (source + 1) * LANES], inner)
                best = jnp.where(outer == source, more, best)
            for n in range(lefts):
                out_ref[0, n, j : j + 1, lanes] = best[n : n + 1]
                out_ref[1, n, j : j + 1, lanes] = best[half + n : half + n + 1]


def finished(own, others, order, place, shape, scale, own_rights):
    count = own_rights + len(others)
    return pl.pallas_call(
        partial(finish_kernel, scale, len(others), own_rights),
        out_shape=jax.ShapeDtypeStruct(shape, F32),
        in_specs=[pl.BlockSpec(memory_space=pltpu.SMEM)]
        + [pl.BlockSpec(memory_space=pltpu.VMEM)] * (2 + len(others)),
        scratch_shapes=[pltpu.VMEM((count, SUB, shape[-1]), F32)],
        compiler_params=pltpu.CompilerParams(vmem_limit_bytes=60000 * 1024),
    )(order, place, own, *others)


def local(left_bands, right_bands, sphere_index, right_order):
    lefts, own_rights, planes = left_bands.shape[1], right_bands.shape[1], left_bands.shape[2]
    length, width = left_bands.shape[3], left_bands.shape[4]
    groups = lax.axis_size("grid")
    me = lax.axis_index("grid")
    per_block = sphere_index.shape[0] // groups
    slots = per_block // groups
    rows = length // groups
    sizes = (groups, slots)
    cuts = [(0, planes)] if planes < 4 else [(0, planes // 2), (planes // 2, planes)]
    routes = [(0, 0, planes)] + [(1, low, high) for low, high in cuts]
    sent = [swapped(right_bands[:, m : m + 1, low:high], "band", 0) for m, low, high in routes]

    wave_z = sphere_index // (length * width)
    wave_y = sphere_index // width % length
    wave_x = sphere_index % width
    spot = jnp.arange(sphere_index.shape[0], dtype=jnp.int32) % per_block
    key = ((wave_y * length + wave_z) * width + wave_x) * per_block + spot
    key = lax.sort(key.reshape(groups, per_block), dimension=1)
    mine = lax.dynamic_slice_in_dim(key, me, 1, 0) % per_block
    back = mine * per_block + jnp.arange(per_block, dtype=jnp.int32)[None]
    place = lax.sort(back, dimension=1) % per_block
    key = jnp.transpose(key.reshape(groups, groups, slots), (1, 0, 2)).reshape(-1, LANES)
    key = key // per_block
    picks = jnp.stack([key % width, key // (width * length) % rows])
    plane_wave = key // width % length

    def turn(z):
        angle = (plane_wave * z % length).astype(F32) * (2.0 * math.pi / length)
        return [jnp.cos(angle), -jnp.sin(angle)]

    tables = (two_terms(rows_table(length)), two_terms(lanes_table(width)))

    def sums(right, low, high, before):
        start = me * planes + low
        turns = jnp.stack(turn(1) + turn(start) + turn(start + (high - low) // 2))
        return chunk_sums(
            left_bands[:, :, low:high], right, tables, picks, turns, before, sizes
        )

    def owned(value):
        return lax.all_to_all(to_owner(value, sizes), "grid", 0, 0, tiled=True)

    own = owned(sums(right_bands, 0, planes, None))
    first = owned(sums(sent[0], 0, planes, None))
    second = None
    for right, (_, low, high) in zip(sent[1:], routes[1:]):
        second = sums(right, low, high, second)
    second = owned(second)
    order = (right_order - lax.axis_index("band") * own_rights) % right_order.shape[0]
    shape = (2, lefts, right_order.shape[0], per_block)
    scale = 1.0 / (length * length * width) ** 0.5
    return finished(own, [first, second], order, place, shape, scale, own_rights)


def solution(mesh):
    placed = (P(None, "band", "grid", None, None), P(None, "band", "grid", None, None), P(), P())
    return jax.shard_map(
        local, mesh=mesh, in_specs=placed, out_specs=P(None, "band", None, "grid"), check_vma=False
    )
```

```python
from functools import partial
import math

import jax
import jax.numpy as jnp
import numpy as np
from jax import lax
from jax.experimental import pallas as pl
from jax.experimental.pallas import tpu as pltpu
from jax.sharding import PartitionSpec as P


F32 = jnp.float32
BF16 = jnp.bfloat16
LANES = 128
SUB = 8
SPAN = 3


def swapped(block, axis, apart):
    count = lax.axis_size(axis)
    route = []
    for low in range(count):
        high = low | 1 << apart
        if high != low and high < count:
            route += [(low, high), (high, low)]
    return lax.ppermute(block, axis, route)


def dft_parts(length):
    counter = np.arange(length)
    angles = (counter[:, None] * counter[None, :] % length) * (2.0 * math.pi / length)
    return np.cos(angles), np.sin(angles)


def two_terms(table):
    high = np.asarray(table, BF16)
    return high, np.asarray(table - np.asarray(high, np.float32), BF16)


def rows_table(length):
    cosine, sine = dft_parts(length)
    return np.block([[cosine, sine], [-sine, cosine]]).astype(np.float32)


def lanes_table(length):
    cosine, sine = dft_parts(length)
    return np.block([[cosine, -sine], [sine, cosine]]).astype(np.float32)


def left_table(table):
    high, low = two_terms(table)
    return jnp.asarray(np.concatenate([high, low, high], axis=1))


def right_table(table):
    high, low = two_terms(table)
    return jnp.asarray(np.concatenate([high, high, low], axis=0))


def split(value):
    high = value.astype(BF16)
    return high, (value - high.astype(F32)).astype(BF16)


def dot(a, b):
    return jnp.dot(a, b, preferred_element_type=F32)


def taken(value, lanes):
    return jnp.take_along_axis(value, lanes, axis=1, mode="promise_in_bounds")


def turned(number, count):
    back = 0
    while count > 1:
        back, number, count = 2 * back + number % 2, number // 2, count // 2
    return back


def chunk_kernel(
    plan, starts_ref, left_ref, right_ref, table_y_ref, table_x_ref, picks_ref, places_ref, turns_ref,
    *rest,
):
    if plan["add"]:
        before_ref, *rest = rest
    out_ref, h_real, h_imag, f_even, f_odd, hold_ref = rest
    lefts, rights, planes = plan["lefts"], plan["rights"], plan["planes"]
    pairs = lefts * rights
    halves, tiles, stride = plan["halves"], plan["tiles"], plan["stride"]
    length, groups, rows, chunks = plan["length"], plan["groups"], plan["rows"], plan["chunks"]
    wide = tiles * SUB

    def transform_rows(z, _):
        if halves == 2:
            slot = (z % tiles) * SUB + (z // tiles) * pairs
        else:
            slot = z * SUB
        for first in range(0, pairs, 2):
            fields = []
            for pair in (first, first + 1):
                m, n = pair // lefts, pair % lefts
                lr, li = left_ref[0, n, z], left_ref[1, n, z]
                rr, ri = right_ref[0, m, z], right_ref[1, m, z]
                fields.append(jnp.concatenate([lr * rr + li * ri, lr * ri - li * rr], axis=0))
            high, low = split(jnp.concatenate(fields, axis=1))
            moved = dot(table_y_ref[...], jnp.concatenate([high, high, low], axis=0))
            for k in range(2):
                spot = pl.ds(slot + first + k, length, stride=stride)
                lanes = slice(k * LANES, (k + 1) * LANES)
                h_real[spot, :] = moved[:length, lanes]
                h_imag[spot, :] = moved[length:, lanes]
        return 0

    lax.fori_loop(0, planes, transform_rows, 0)

    def transform_lanes(group, f_ref):
        spots = [pl.ds((group * rows + y) * stride, wide) for y in range(rows)]
        real = jnp.concatenate([h_real[spot, :] for spot in spots], axis=0)
        imag = jnp.concatenate([h_imag[spot, :] for spot in spots], axis=0)
        high, low = split(jnp.concatenate([real, imag], axis=1))
        moved = dot(jnp.concatenate([high, low, high], axis=1), table_x_ref[...])
        for y in range(rows):
            f_ref[y] = moved[y * wide : (y + 1) * wide]

    upper = lax.broadcasted_iota(jnp.int32, (SUB, LANES), 0) >= SUB // 2
    late = lax.broadcasted_iota(jnp.int32, (SUB, LANES), 1) >= LANES // 2
    span = plan["span"]

    def wide_row(ref, at, *k):
        return jnp.broadcast_to(ref[k + (pl.ds(at, 1), slice(None))], (SUB, LANES))

    def box(y, tile, part):
        rows_of, lanes_of = pl.ds(tile * SUB, SUB), pl.ds(part * LANES, LANES)
        return (y, rows_of, lanes_of)

    def near(at, f_ref):
        lanes = wide_row(picks_ref, at, 0)
        start = starts_ref[at]
        apart = wide_row(picks_ref, at, 1) - start
        same = [apart == y for y in range(span)]

        def value(tile, part):
            best = taken(f_ref[box(start, tile, part)], lanes)
            for y in range(1, span):
                best = jnp.where(same[y], taken(f_ref[box(start + y, tile, part)], lanes), best)
            return best

        return value

    def far(at, f_ref):
        lanes = wide_row(picks_ref, at, 0)
        y_of = wide_row(picks_ref, at, 1)

        def value(tile, part):
            def body(y, best):
                return jnp.where(y_of == y, taken(f_ref[box(y, tile, part)], lanes), best)

            return lax.fori_loop(0, rows, body, jnp.zeros((SUB, LANES), F32))

        return value

    def picked(at, value):
        turn_r, turn_i = wide_row(turns_ref, at, 0), wide_row(turns_ref, at, 1)
        base_r, base_i = wide_row(turns_ref, at, 2), wide_row(turns_ref, at, 3)
        if halves == 2:
            base_r = jnp.where(upper, wide_row(turns_ref, at, 4), base_r)
            base_i = jnp.where(upper, wide_row(turns_ref, at, 5), base_i)
        real, imag = value(tiles - 1, 0), value(tiles - 1, 1)
        for tile in reversed(range(tiles - 1)):
            real, imag = (
                real * turn_r - imag * turn_i + value(tile, 0),
                real * turn_i + imag * turn_r + value(tile, 1),
            )
        real, imag = real * base_r - imag * base_i, real * base_i + imag * base_r
        if pairs == SUB:
            found = [real, imag]
        else:
            if halves == 2:
                real = real + pltpu.roll(real, SUB // 2, 0)
                imag = imag + pltpu.roll(imag, SUB // 2, 0)
            else:
                imag = pltpu.roll(imag, SUB // 2, 0)
            found = [jnp.where(upper, imag, real)]
        if plan["add"]:
            found = [one + before_ref[at, part] for part, one in enumerate(found)]
        return found

    def moved_back(group, found):
        result = []
        for chunk in range(chunks):
            place = wide_row(places_ref, group * chunks + chunk)
            lanes, source = place % LANES, place // LANES
            parts = []
            for part in range(len(found[0])):
                best = taken(found[0][part], lanes)
                for other in range(1, chunks):
                    best = jnp.where(source == other, taken(found[other][part], lanes), best)
                parts.append(best)
            result.append(parts)
        return result

    def group_sums(group, f_ref, look):
        found = []
        for chunk in range(chunks):
            at = group * chunks + chunk
            found.append(picked(at, look(at, f_ref)))
        if not plan["last"]:
            for chunk in range(chunks):
                for part, value in enumerate(found[chunk]):
                    out_ref[group * chunks + chunk, part] = value
            return found
        return moved_back(group, found)

    def put_couple(a, firsts, seconds):
        place = pl.ds(pl.multiple_of(a * LANES, LANES), LANES)
        for chunk in range(chunks):
            for part, (one, two) in enumerate(zip(firsts[chunk], seconds[chunk])):
                low, high = turned(2 * chunk, groups), turned(2 * chunk + 1, groups)
                out_ref[low, part, :, place] = jnp.where(late, pltpu.roll(two, LANES // 2, 1), one)
                out_ref[high, part, :, place] = jnp.where(late, two, pltpu.roll(one, LANES // 2, 1))

    def put_single(group, found):
        for chunk in range(chunks):
            for part, value in enumerate(found[chunk]):
                out_ref[group * chunks + chunk, part] = value

    @pl.when(starts_ref[groups * chunks] == 1)
    def _():
        if groups % 2:

            def single(group, _):
                transform_lanes(group, f_even)
                found = group_sums(group, f_even, near)
                if plan["last"]:
                    put_single(group, found)
                return 0

            lax.fori_loop(0, groups, single, 0)
            return
        transform_lanes(0, f_even)

        def couple(a, _):
            transform_lanes(2 * a + 1, f_odd)
            firsts = group_sums(2 * a, f_even, near)
            transform_lanes(jnp.minimum(2 * a + 2, groups - 1), f_even)
            seconds = group_sums(2 * a + 1, f_odd, near)
            if plan["last"]:
                if plan["woven"]:
                    put_couple(a, firsts, seconds)
                else:
                    put_single(2 * a, firsts)
                    put_single(2 * a + 1, seconds)
            return 0

        lax.fori_loop(0, groups // 2, couple, 0)

    @pl.when(starts_ref[groups * chunks] == 0)
    def _():
        def compute(group):
            transform_lanes(group, f_even)

            def body(chunk, _):
                at = group * chunks + chunk
                for part, value in enumerate(picked(at, far(at, f_even))):
                    hold_ref[chunk, part] = value
                return 0

            lax.fori_loop(0, chunks, body, 0)
            count = 2 if pairs == SUB else 1
            found = [[hold_ref[chunk, part] for part in range(count)] for chunk in range(chunks)]
            return moved_back(group, found) if plan["last"] else found

        if plan["last"] and plan["woven"]:

            def couple(a, _):
                firsts = compute(2 * a)
                put_couple(a, firsts, compute(2 * a + 1))
                return 0

            lax.fori_loop(0, groups // 2, couple, 0)
        else:

            def single(group, _):
                put_single(group, compute(group))
                return 0

            lax.fori_loop(0, groups, single, 0)


def is_woven(sizes):
    groups, slots = sizes
    return 2 * slots == LANES and groups % 2 == 0


def chunk_sums(left, right, tables, lists, turns, before, last, sizes):
    lefts, rights = left.shape[1], right.shape[1]
    planes, length = left.shape[2], left.shape[3]
    groups, slots = sizes
    pairs = lefts * rights
    halves = 2 if pairs < SUB and planes % 2 == 0 else 1
    tiles = planes // halves
    wide = tiles * SUB
    stride = wide if tiles % 2 else wide + SUB
    parts = 2 * pairs // SUB
    chunks = groups * slots // LANES
    woven = is_woven(sizes)
    plan = dict(
        lefts=lefts, rights=rights, planes=planes, halves=halves, tiles=tiles, stride=stride,
        length=length, groups=groups, rows=length // groups, chunks=chunks, woven=woven,
        add=before is not None, last=last, span=min(SPAN, length // groups),
    )
    if woven and last:
        shape = (groups, parts, SUB, groups * slots)
    else:
        shape = (groups * chunks, parts, SUB, LANES)
    starts, picks, places = lists
    operands = [starts, left, right, *tables, picks, places, turns]
    if before is not None:
        operands.append(before)
    field = pltpu.VMEM((length * stride, LANES), F32)
    group = pltpu.VMEM((length // groups, wide, 2 * LANES), F32)
    flops = 2 * 3 * 2 * pairs * planes * length * (2 * length) * (2 * length)
    return pl.pallas_call(
        partial(chunk_kernel, plan),
        out_shape=jax.ShapeDtypeStruct(shape, F32),
        in_specs=[pl.BlockSpec(memory_space=pltpu.SMEM)]
        + [pl.BlockSpec(memory_space=pltpu.VMEM)] * (len(operands) - 1),
        scratch_shapes=[field, field, group, group, pltpu.VMEM((chunks, parts, SUB, LANES), F32)],
        compiler_params=pltpu.CompilerParams(vmem_limit_bytes=58 * 1024 * 1024),
        cost_estimate=pl.CostEstimate(flops=flops, bytes_accessed=4 * left.size, transcendentals=0),
    )(*operands)


def to_owner(sums, sizes):
    groups, slots = sizes
    if is_woven(sizes):
        return sums
    parts = sums.shape[1]
    shaped = sums.reshape(groups, -1, parts, SUB, LANES)
    shaped = jnp.moveaxis(shaped, 1, 3).reshape(groups, parts, SUB, groups, slots)
    shaped = jnp.transpose(shaped, (3, 1, 2, 0, 4)).reshape(groups, parts, SUB, groups * slots)
    return shaped[np.array([turned(owner, groups) for owner in range(groups)])]


def halved_sum(sums, axis):
    count = sums.shape[0]
    me = lax.axis_index(axis)
    apart = 1
    while sums.shape[0] > 1:
        half = sums.shape[0] // 2
        side = me // apart % 2
        sent = lax.dynamic_slice_in_dim(sums, (1 - side) * half, half, 0)
        kept = lax.dynamic_slice_in_dim(sums, side * half, half, 0)
        route = [(device, device ^ apart) for device in range(count)]
        sums = kept + lax.ppermute(sent, axis, route)
        apart *= 2
    return sums


def order_kernel(subs, key_ref, sorted_ref, place_ref):
    size, width = key_ref.shape[1], key_ref.shape[0]
    total = size * subs
    row = lax.broadcasted_iota(jnp.int32, (size, width), 0)
    lane = lax.broadcasted_iota(jnp.int32, (size, width), 1)
    spot = lane % subs * size + row

    def sort(value):
        span = 2
        while span <= total:
            apart = span // 2
            rising = spot & span == 0
            while apart > 0:
                first = spot & apart == 0
                if apart < size:
                    axis, shift, full = 0, apart, size
                else:
                    axis, shift, full = 1, apart // size, width
                other = jnp.where(
                    first, pltpu.roll(value, full - shift, axis), pltpu.roll(value, shift, axis)
                )
                small, large = jnp.minimum(value, other), jnp.maximum(value, other)
                value = jnp.where(first == rising, small, large)
                apart //= 2
            span *= 2
        return value

    value = sort(key_ref[...].T)
    sorted_ref[...] = value.T
    back = sort(value % total * total + spot)
    place_ref[...] = (back % total).T


def ordered(key, per_block):
    shape = (key.size // LANES, LANES)
    like = jax.ShapeDtypeStruct(shape, jnp.int32)
    return pl.pallas_call(
        partial(order_kernel, per_block // LANES), out_shape=[like, like]
    )(key.reshape(shape))


def finish_kernel(scale, count, own_rights, order_ref, place_ref, own_ref, *rest):
    others, out_ref, hold_ref = rest[:count], rest[count], rest[count + 1]
    length = out_ref.shape[-1]
    lefts = out_ref.shape[1]
    half = SUB // 2

    def total(ref, part):
        value = ref[0, part]
        for source in range(1, ref.shape[0]):
            value = value + ref[source, part]
        return value * scale

    blocks = [[total(own_ref, part) for part in range(own_ref.shape[1])]]
    if len(blocks[0]) == 2:
        real, imag = blocks[0]
        for m in range(own_rights):
            rows = slice(m * lefts, (m + 1) * lefts)
            hold_ref[m] = jnp.concatenate([real[rows], imag[rows]], axis=0)
    for k, ref in enumerate(others):
        hold_ref[own_rights + k] = total(ref, 0)
    pieces = length // LANES
    for j in range(out_ref.shape[2]):
        block = hold_ref[order_ref[j]]
        for piece in range(pieces):
            lanes = slice(piece * LANES, (piece + 1) * LANES)
            place = jnp.broadcast_to(place_ref[:, lanes], (SUB, LANES))
            inner = place % LANES
            outer = place // LANES
            best = taken(block[:, :LANES], inner)
            for source in range(1, pieces):
                more = taken(block[:, source * LANES : (source + 1) * LANES], inner)
                best = jnp.where(outer == source, more, best)
            for n in range(lefts):
                out_ref[0, n, j : j + 1, lanes] = best[n : n + 1]
                out_ref[1, n, j : j + 1, lanes] = best[half + n : half + n + 1]


def finished(own, others, order, place, shape, scale, own_rights):
    count = own_rights + len(others)
    return pl.pallas_call(
        partial(finish_kernel, scale, len(others), own_rights),
        out_shape=jax.ShapeDtypeStruct(shape, F32),
        in_specs=[pl.BlockSpec(memory_space=pltpu.SMEM)]
        + [pl.BlockSpec(memory_space=pltpu.VMEM)] * (2 + len(others)),
        scratch_shapes=[pltpu.VMEM((count, SUB, shape[-1]), F32)],
        compiler_params=pltpu.CompilerParams(vmem_limit_bytes=58 * 1024 * 1024),
    )(order, place, own, *others)


def local(left_bands, right_bands, sphere_index, right_order):
    lefts, own_rights, planes = left_bands.shape[1], right_bands.shape[1], left_bands.shape[2]
    length, width = left_bands.shape[3], left_bands.shape[4]
    groups = lax.axis_size("grid")
    me = lax.axis_index("grid")
    per_block = sphere_index.shape[0] // groups
    slots = per_block // groups
    rows = length // groups
    sizes = (groups, slots)
    cuts = [(0, planes)] if planes < 4 else [(0, planes // 2), (planes // 2, planes)]
    routes = [(0, 0, planes)] + [(1, low, high) for low, high in cuts]
    sent = []
    for m, low, high in routes:
        sent.append(swapped(right_bands[:, m : m + 1, low:high], "band", 0))

    wave_z = sphere_index // (length * width)
    wave_y = sphere_index // width % length
    wave_x = sphere_index % width
    spot = jnp.arange(sphere_index.shape[0], dtype=jnp.int32) % per_block
    key = ((wave_y * length + wave_z) * width + wave_x) * per_block + spot
    key, place = ordered(key, per_block)
    place = lax.dynamic_slice_in_dim(place.reshape(groups, per_block), me, 1, 0)
    key = jnp.transpose(key.reshape(groups, groups, slots), (1, 0, 2)) // per_block
    spot = jnp.arange(groups * slots, dtype=jnp.int32).reshape(groups, slots)
    key, places = ordered((key % (rows * length * width)) * (groups * slots) + spot, groups * slots)
    key = key // (groups * slots)
    row_of = key // (width * length)
    picks = jnp.stack([key % width, row_of])
    starts = jnp.clip(row_of[:, 0], 0, rows - min(SPAN, rows))
    near = jnp.all(row_of[:, -1] - starts < SPAN).astype(jnp.int32)
    lists = (jnp.concatenate([starts, near[None]]), picks, places)
    plane_wave = key // width % length

    def turn(z):
        angle = (plane_wave * z % length).astype(F32) * (2.0 * math.pi / length)
        return [jnp.cos(angle), -jnp.sin(angle)]

    tables = (left_table(rows_table(length)), right_table(lanes_table(width)))

    def sums(right, low, high, before, last):
        start = me * planes + low
        turns = jnp.stack(turn(1) + turn(start) + turn(start + (high - low) // 2))
        return chunk_sums(
            left_bands[:, :, low:high], right, tables, lists, turns, before, last, sizes
        )

    def owned(value):
        return halved_sum(to_owner(value, sizes), "grid")

    own_sums = sums(right_bands, 0, planes, None, True)
    right, _ = lax.optimization_barrier((sent[0], own_sums))
    first_sums = sums(right, 0, planes, None, True)
    last_sums, ahead = None, first_sums
    for right, (_, low, high) in zip(sent[1:], routes[1:]):
        right, _ = lax.optimization_barrier((right, ahead))
        last_sums = ahead = sums(right, low, high, last_sums, high == planes)
    own, first, second = owned(own_sums), owned(first_sums), owned(last_sums)
    order = (right_order - lax.axis_index("band") * own_rights) % right_order.shape[0]
    shape = (2, lefts, right_order.shape[0], per_block)
    scale = 1.0 / (length * length * width) ** 0.5
    return finished(own, [first, second], order, place, shape, scale, own_rights)


def solution(mesh):
    placed = (P(None, "band", "grid", None, None), P(None, "band", "grid", None, None), P(), P())
    return jax.shard_map(
        local, mesh=mesh, in_specs=placed, out_specs=P(None, "band", None, "grid"), check_vma=False
    )
```

```python
from functools import partial
import math

import jax
import jax.numpy as jnp
import numpy as np
from jax import lax
from jax.experimental import pallas as pl
from jax.experimental.pallas import tpu as pltpu
from jax.sharding import PartitionSpec as P


F32 = jnp.float32
BF16 = jnp.bfloat16
LANES = 128
SUB = 8
SPAN = 3
VMEM_MIB = 16


def swapped(block, axis, apart):
    count = lax.axis_size(axis)
    route = []
    for low in range(count):
        high = low | 1 << apart
        if high != low and high < count:
            route += [(low, high), (high, low)]
    return lax.ppermute(block, axis, route)


def dft_parts(length):
    counter = np.arange(length)
    angles = (counter[:, None] * counter[None, :] % length) * (2.0 * math.pi / length)
    return np.cos(angles), np.sin(angles)


def two_terms(table):
    high = np.asarray(table, BF16)
    return high, np.asarray(table - np.asarray(high, np.float32), BF16)


def rows_table(length):
    cosine, sine = dft_parts(length)
    return np.block([[cosine, sine], [-sine, cosine]]).astype(np.float32)


def lanes_table(length):
    cosine, sine = dft_parts(length)
    return np.block([[cosine, -sine], [sine, cosine]]).astype(np.float32)


def left_table(table):
    high, low = two_terms(table)
    return jnp.asarray(np.concatenate([high, low, high], axis=1))


def right_table(table):
    high, low = two_terms(table)
    return jnp.asarray(np.concatenate([high, high, low], axis=0))


def split(value):
    high = value.astype(BF16)
    return high, (value - high.astype(F32)).astype(BF16)


def dot(a, b):
    return jnp.dot(a, b, preferred_element_type=F32)


def taken(value, lanes):
    return jnp.take_along_axis(value, lanes, axis=1, mode="promise_in_bounds")


def turned(number, count):
    back = 0
    while count > 1:
        back, number, count = 2 * back + number % 2, number // 2, count // 2
    return back


def window(chunk, chunks, rows):
    return min(max(chunk * rows // chunks - 1, 0), rows - min(SPAN, rows))


def half_planes(pairs, planes):
    return planes // 2 if pairs < SUB and planes % 2 == 0 else planes


def chunk_kernel(
    plan, near_ref, left_ref, right_ref, table_y_ref, table_x_ref, picks_ref, places_ref, turns_ref,
    *rest,
):
    if plan["add"]:
        before_ref, *rest = rest
    if plan["join"]:
        other_kept_ref, other_sent_ref, *rest = rest
    out_ref, *rest = rest
    if plan["woven"] and plan["last"]:
        send_ref, *rest = rest
    skip = plan["join"]
    for part in range(skip):
        for spot in range(out_ref.shape[0]):
            out_ref[spot, part] = other_kept_ref[spot, part]
            send_ref[spot, part] = other_sent_ref[spot, part]
    h_real, h_imag, f_even, f_odd, hold_ref, *d_refs = rest
    lefts, rights, planes = plan["lefts"], plan["rights"], plan["planes"]
    pairs = lefts * rights
    halves, tiles, stride = plan["halves"], plan["tiles"], plan["stride"]
    length, groups, rows, chunks = plan["length"], plan["groups"], plan["rows"], plan["chunks"]
    wide = tiles * SUB
    left_low, right_low = plan["low"], plan["right_low"]

    def transform_rows(z, _):
        if halves == 2:
            slot = (z % tiles) * SUB + (z // tiles) * pairs
        else:
            slot = z * SUB
        for first in range(0, pairs, 2):
            d_ref = d_refs[first // 2]
            for k in range(2):
                m, n = (first + k) // lefts, (first + k) % lefts
                lanes = slice(k * LANES, (k + 1) * LANES)
                lr, li = left_ref[0, n, left_low + z], left_ref[1, n, left_low + z]
                rr, ri = right_ref[0, m, right_low + z], right_ref[1, m, right_low + z]
                for part, field in enumerate((lr * rr + li * ri, lr * ri - li * rr)):
                    high, low = split(field)
                    for copy, term in enumerate((high, high, low)):
                        base = (2 * copy + part) * length
                        d_ref[base : base + length, lanes] = term
            moved = dot(table_y_ref[...], d_ref[...])
            for k in range(2):
                spot = pl.ds(slot + first + k, length, stride=stride)
                lanes = slice(k * LANES, (k + 1) * LANES)
                h_real[spot, :] = moved[:length, lanes]
                h_imag[spot, :] = moved[length:, lanes]
        return 0

    lax.fori_loop(0, planes, transform_rows, 0)

    def transform_lanes(group, f_ref):
        spots = [pl.ds((group * rows + y) * stride, wide) for y in range(rows)]
        real = jnp.concatenate([h_real[spot, :] for spot in spots], axis=0)
        imag = jnp.concatenate([h_imag[spot, :] for spot in spots], axis=0)
        high, low = split(jnp.concatenate([real, imag], axis=1))
        moved = dot(jnp.concatenate([high, low, high], axis=1), table_x_ref[...])
        for y in range(rows):
            f_ref[y] = moved[y * wide : (y + 1) * wide]

    upper = lax.broadcasted_iota(jnp.int32, (SUB, LANES), 0) >= SUB // 2
    late = lax.broadcasted_iota(jnp.int32, (SUB, LANES), 1) >= LANES // 2
    span = plan["span"]

    def wide_row(ref, at, *k):
        return jnp.broadcast_to(ref[k + (pl.ds(at, 1), slice(None))], (SUB, LANES))

    def box(y, tile, part):
        rows_of, lanes_of = pl.ds(tile * SUB, SUB), pl.ds(part * LANES, LANES)
        return (y, rows_of, lanes_of)

    def near(chunk, at, f_ref):
        lanes = wide_row(picks_ref, at, 0)
        start = window(chunk, chunks, rows)
        apart = wide_row(picks_ref, at, 1) - start
        same = [apart == y for y in range(span)]

        def value(tile, part):
            best = taken(f_ref[box(start, tile, part)], lanes)
            for y in range(1, span):
                best = jnp.where(same[y], taken(f_ref[box(start + y, tile, part)], lanes), best)
            return best

        return value

    def far(at, f_ref):
        lanes = wide_row(picks_ref, at, 0)
        y_of = wide_row(picks_ref, at, 1)

        def value(tile, part):
            def body(y, best):
                return jnp.where(y_of == y, taken(f_ref[box(y, tile, part)], lanes), best)

            return lax.fori_loop(0, rows, body, jnp.zeros((SUB, LANES), F32))

        return value

    def picked(at, value):
        first_turn, second_turn = plan["turns"]
        turn_r, turn_i = wide_row(turns_ref, at, 0, 0), wide_row(turns_ref, at, 0, 1)
        base_r = wide_row(turns_ref, at, first_turn, 0)
        base_i = wide_row(turns_ref, at, first_turn, 1)
        if halves == 2:
            base_r = jnp.where(upper, wide_row(turns_ref, at, second_turn, 0), base_r)
            base_i = jnp.where(upper, wide_row(turns_ref, at, second_turn, 1), base_i)
        real, imag = value(tiles - 1, 0), value(tiles - 1, 1)
        for tile in reversed(range(tiles - 1)):
            real, imag = (
                real * turn_r - imag * turn_i + value(tile, 0),
                real * turn_i + imag * turn_r + value(tile, 1),
            )
        real, imag = real * base_r - imag * base_i, real * base_i + imag * base_r
        if pairs == SUB:
            found = [real, imag]
        else:
            if halves == 2:
                real = real + pltpu.roll(real, SUB // 2, 0)
                imag = imag + pltpu.roll(imag, SUB // 2, 0)
            else:
                imag = pltpu.roll(imag, SUB // 2, 0)
            found = [jnp.where(upper, imag, real)]
        if plan["add"]:
            found = [one + before_ref[at, part] for part, one in enumerate(found)]
        return found

    def moved_back(group, found):
        result = []
        for chunk in range(chunks):
            place = wide_row(places_ref, group * chunks + chunk)
            lanes, source = place % LANES, place // LANES
            parts = []
            for part in range(len(found[0])):
                best = taken(found[0][part], lanes)
                for other in range(1, chunks):
                    best = jnp.where(source == other, taken(found[other][part], lanes), best)
                parts.append(best)
            result.append(parts)
        return result

    def group_sums(group, f_ref, look):
        found = []
        for chunk in range(chunks):
            at = group * chunks + chunk
            found.append(picked(at, look(chunk, at, f_ref)))
        if not plan["last"]:
            for chunk in range(chunks):
                for part, value in enumerate(found[chunk]):
                    out_ref[group * chunks + chunk, part] = value
            return found
        return moved_back(group, found)

    def put_couple(a, firsts, seconds):
        place = pl.ds(pl.multiple_of(a * LANES, LANES), LANES)
        for chunk in range(chunks):
            for part, (one, two) in enumerate(zip(firsts[chunk], seconds[chunk])):
                spot = turned(2 * chunk, groups)
                box_of = (spot, skip + part, slice(None), place)
                out_ref[box_of] = jnp.where(late, pltpu.roll(two, LANES // 2, 1), one)
                send_ref[box_of] = jnp.where(late, two, pltpu.roll(one, LANES // 2, 1))

    def put_single(group, found):
        for chunk in range(chunks):
            for part, value in enumerate(found[chunk]):
                out_ref[group * chunks + chunk, part] = value

    @pl.when(near_ref[0] == 1)
    def _():
        if groups % 2:

            def single(group, _):
                transform_lanes(group, f_even)
                found = group_sums(group, f_even, near)
                if plan["last"]:
                    put_single(group, found)
                return 0

            lax.fori_loop(0, groups, single, 0)
            return
        transform_lanes(0, f_even)

        def couple(a, _):
            transform_lanes(2 * a + 1, f_odd)
            firsts = group_sums(2 * a, f_even, near)
            transform_lanes(jnp.minimum(2 * a + 2, groups - 1), f_even)
            seconds = group_sums(2 * a + 1, f_odd, near)
            if plan["last"]:
                if plan["woven"]:
                    put_couple(a, firsts, seconds)
                else:
                    put_single(2 * a, firsts)
                    put_single(2 * a + 1, seconds)
            return 0

        lax.fori_loop(0, groups // 2, couple, 0)

    @pl.when(near_ref[0] == 0)
    def _():
        def compute(group):
            transform_lanes(group, f_even)

            def body(chunk, _):
                at = group * chunks + chunk
                for part, value in enumerate(picked(at, far(at, f_even))):
                    hold_ref[chunk, part] = value
                return 0

            lax.fori_loop(0, chunks, body, 0)
            count = 2 if pairs == SUB else 1
            found = [[hold_ref[chunk, part] for part in range(count)] for chunk in range(chunks)]
            return moved_back(group, found) if plan["last"] else found

        if plan["last"] and plan["woven"]:

            def couple(a, _):
                firsts = compute(2 * a)
                put_couple(a, firsts, compute(2 * a + 1))
                return 0

            lax.fori_loop(0, groups // 2, couple, 0)
        else:

            def single(group, _):
                put_single(group, compute(group))
                return 0

            lax.fori_loop(0, groups, single, 0)


def is_woven(sizes):
    groups, slots = sizes
    return 2 * slots == LANES and groups % 2 == 0


def chunk_sums(left, right, tables, lists, before, join, last, sizes, spans):
    lefts, rights, length = left.shape[1], right.shape[1], left.shape[3]
    groups, slots = sizes
    low, right_low, planes, turns = spans
    pairs = lefts * rights
    tiles = half_planes(pairs, planes)
    wide = tiles * SUB
    stride = wide if tiles % 2 else wide + SUB
    parts = 2 * pairs // SUB
    chunks = groups * slots // LANES
    rows = length // groups
    operands = [left, right, *tables, *lists[1:]]
    if before is not None:
        operands.append(before)
    if join is not None and not is_woven(sizes):
        mine = chunk_sums(left, right, tables, lists, before, None, last, sizes, spans)
        return jnp.concatenate([join, mine], axis=1)
    if join is not None:
        operands += list(join)
    skip = 0 if join is None else join[0].shape[1]
    plan = dict(
        lefts=lefts, rights=rights, planes=planes, halves=planes // tiles, tiles=tiles,
        stride=stride, length=length, groups=groups, rows=rows, chunks=chunks,
        woven=is_woven(sizes), add=before is not None, last=last, span=min(SPAN, rows),
        low=low, right_low=right_low, turns=turns, join=skip,
    )
    if is_woven(sizes) and last:
        shape = (groups // 2, skip + parts, SUB, groups * slots)
    else:
        shape = (groups * chunks, parts, SUB, LANES)
    like = jax.ShapeDtypeStruct(shape, F32)
    field = pltpu.VMEM((length * stride, LANES), F32)
    group = pltpu.VMEM((rows, wide, 2 * LANES), F32)
    flops = 2 * 3 * 2 * pairs * planes * length * (2 * length) * (2 * length)
    return pl.pallas_call(
        partial(chunk_kernel, plan),
        out_shape=[like, like] if is_woven(sizes) and last else like,
        in_specs=[pl.BlockSpec(memory_space=pltpu.SMEM)]
        + [pl.BlockSpec(memory_space=pltpu.VMEM)] * len(operands),
        scratch_shapes=[field, field, group, group, pltpu.VMEM((chunks, parts, SUB, LANES), F32)]
        + [pltpu.VMEM((6 * length, 2 * LANES), BF16)] * (pairs // 2),
        compiler_params=pltpu.CompilerParams(vmem_limit_bytes=VMEM_MIB * 1024 * 1024),
        cost_estimate=pl.CostEstimate(flops=flops, bytes_accessed=4 * left.size, transcendentals=0),
    )(lists[0], *operands)


def to_owner(sums, sizes):
    if is_woven(sizes):
        return sums
    groups, slots = sizes
    parts = sums.shape[1]
    shaped = sums.reshape(groups, -1, parts, SUB, LANES)
    shaped = jnp.moveaxis(shaped, 1, 3).reshape(groups, parts, SUB, groups, slots)
    shaped = jnp.transpose(shaped, (3, 1, 2, 0, 4)).reshape(groups, parts, SUB, groups * slots)
    shaped = shaped[np.array([turned(owner, groups) for owner in range(groups)])]
    return shaped[: groups // 2], shaped[groups // 2 :]


def add_kernel(kept_ref, got_ref, *out_refs):
    share = kept_ref.shape[0] // len(out_refs)
    for k, out_ref in enumerate(out_refs):
        for one in range(share):
            out_ref[one] = kept_ref[k * share + one] + got_ref[k * share + one]


def added(kept, got, pieces):
    like = jax.ShapeDtypeStruct((kept.shape[0] // pieces,) + kept.shape[1:], F32)
    return pl.pallas_call(
        add_kernel,
        out_shape=[like] * pieces,
        compiler_params=pltpu.CompilerParams(vmem_limit_bytes=8 * 1024 * 1024),
    )(kept, got)


def grid_parts(kept, sent, axis):
    count = 2 * kept.shape[0]
    step = 0

    def moved(value, apart):
        route = [(device, device ^ apart) for device in range(count)]
        return lax.ppermute(value, axis, route)

    while kept.shape[0] > 4:
        got = moved(sent, 1 << step)
        kept, sent = added(kept, got, 2)
        step += 1
    got = moved(sent, 1 << step)
    kept, *sent = added(kept, got, kept.shape[0])
    low, high = 2 << step, 4 << step
    step += 1
    aparts = [high, low, low | high] if len(sent) == 3 else [low] * len(sent)
    return [kept] + [moved(one, apart) for one, apart in zip(sent, aparts)]


def over(value, count):
    if count & count - 1 == 0:
        return value >> count.bit_length() - 1
    return value // count


def rest_of(value, count):
    if count & count - 1 == 0:
        return value & count - 1
    return value % count


def list_kernel(
    plan, me_ref, index_ref, table_ref, near_ref, place_ref, picks_ref, places_ref, turns_ref, hold_ref
):
    groups, slots, rows, chunks = plan["groups"], plan["slots"], plan["rows"], plan["chunks"]
    length, width = plan["length"], plan["width"]
    size, lanes = index_ref.shape[1], index_ref.shape[0]
    total = groups * slots
    subs = total // size
    row = lax.broadcasted_iota(jnp.int32, (size, lanes), 0)
    lane = lax.broadcasted_iota(jnp.int32, (size, lanes), 1)
    spot = rest_of(lane, subs) * size + row
    flat_spot = rest_of(row, subs) * size + lane
    me = me_ref[0]

    def sort(value):
        span = 2
        while span <= total:
            apart = span // 2
            rising = spot & span == 0
            while apart > 0:
                first = spot & apart == 0
                if apart < size:
                    axis, shift, full = 0, apart, size
                else:
                    axis, shift, full = 1, apart // size, lanes
                other = jnp.where(
                    first, pltpu.roll(value, full - shift, axis), pltpu.roll(value, shift, axis)
                )
                small, large = jnp.minimum(value, other), jnp.maximum(value, other)
                value = jnp.where(first == rising, small, large)
                apart //= 2
            span *= 2
        return value

    index = index_ref[...]
    wave_z = over(index, length * width)
    wave_y = rest_of(over(index, width), length)
    wave_x = rest_of(index, width)
    key = ((wave_y * length + wave_z) * width + wave_x) * total + flat_spot
    key = key.T
    hold_ref[...] = key.T
    mine = pltpu.roll(key, lanes - me * subs, 1)
    for sub in range(subs):
        own = jnp.broadcast_to(hold_ref[pl.ds(me * subs + sub, 1), :], (SUB, lanes))
        count = jnp.zeros((SUB, lanes), jnp.int32)
        for other in range(subs):
            column = jnp.broadcast_to(mine[:, other : other + 1], (size, lanes))
            for low in range(0, size, SUB):
                count = count + (column[low : low + SUB] < own).astype(jnp.int32)
        place_ref[:, sub * size : (sub + 1) * size] = jnp.sum(count, axis=0, keepdims=True)

    hold_ref[...] = over(sort(key), total).T
    if slots == 1:
        key = hold_ref[...]
    else:
        half = size // 2
        late = lax.broadcasted_iota(jnp.int32, (groups // 2, size), 1) >= half
        for pair in range(groups // 2):
            even = hold_ref[pl.ds(pair, groups // 2, stride=2 * subs), :]
            odd = hold_ref[pl.ds(subs + pair, groups // 2, stride=2 * subs), :]
            low = jnp.where(late, pltpu.roll(odd, half, 1), even)
            high = jnp.where(late, odd, pltpu.roll(even, half, 1))
            places_ref[pl.ds(2 * pair * subs, subs), :] = low
            places_ref[pl.ds((2 * pair + 1) * subs, subs), :] = high
        key = places_ref[...].T
    key = sort(rest_of(key, rows * length * width) * total + spot)
    hold_ref[...] = rest_of(sort(rest_of(key, total) * total + spot), total).T
    sharing = LANES // slots
    swap = lax.broadcasted_iota(jnp.int32, (groups, LANES), 1) ^ (rest_of(me, sharing) * slots)
    for chunk in range(chunks):
        other = chunk ^ over(me, sharing)
        value = hold_ref[pl.ds(other, groups, stride=chunks), :] if chunks > 1 else hold_ref[...]
        value = jnp.concatenate(
            [
                taken(value[low : low + SUB], swap[low : low + SUB])
                for low in range(0, groups, SUB)
            ],
            axis=0,
        )
        if chunks > 1:
            places_ref[pl.ds(chunk, groups, stride=chunks), :] = value
        else:
            places_ref[...] = value
    key = over(key, total).T
    row_of = over(key, width * length)
    chunk = rest_of(row, chunks)
    start = jnp.zeros_like(row)
    for k in range(chunks):
        start = jnp.where(chunk == k, window(k, chunks, rows), start)
    apart = row_of - start
    outside = (apart < 0) | (apart >= SPAN)
    near_ref[0] = 1 - jnp.max(outside.astype(F32)).astype(jnp.int32)
    picks_ref[0] = rest_of(key, width)
    picks_ref[1] = row_of
    wave_z = rest_of(over(key, width), length)
    cosine, sine = table_ref[0:1, :], table_ref[1:2, :]
    for k, offset in enumerate(plan["offsets"]):
        plane = 1 if k == 0 else me * plan["planes"] + offset
        angle = rest_of(wave_z * plane, length)
        for low in range(0, lanes, SUB):
            at = angle[low : low + SUB]
            turns_ref[k, 0, low : low + SUB] = taken(jnp.broadcast_to(cosine, (SUB, length)), at)
            turns_ref[k, 1, low : low + SUB] = taken(jnp.broadcast_to(sine, (SUB, length)), at)


def listed(sphere_index, me, length, width, planes, sizes, offsets):
    groups, slots = sizes
    total = groups * slots
    shape = (sphere_index.size // LANES, LANES)
    plan = dict(
        groups=groups, slots=slots, rows=length // groups, chunks=total // LANES, length=length,
        width=width, planes=planes, offsets=offsets,
    )
    counter = np.arange(length) * (2.0 * math.pi / length)
    table = jnp.asarray(np.stack([np.cos(counter), -np.sin(counter)]), F32)
    spec, small = pl.BlockSpec(memory_space=pltpu.VMEM), pl.BlockSpec(memory_space=pltpu.SMEM)
    whole = jax.ShapeDtypeStruct(shape, jnp.int32)
    return pl.pallas_call(
        partial(list_kernel, plan),
        out_shape=[
            jax.ShapeDtypeStruct((1,), jnp.int32),
            jax.ShapeDtypeStruct((1, total), jnp.int32),
            jax.ShapeDtypeStruct((2,) + shape, jnp.int32),
            whole,
            jax.ShapeDtypeStruct((len(offsets), 2) + shape, F32),
        ],
        in_specs=[small, spec, spec],
        out_specs=[small, spec, spec, spec, spec],
        scratch_shapes=[pltpu.VMEM(shape, jnp.int32)],
        cost_estimate=pl.CostEstimate(flops=10**10, bytes_accessed=10**6, transcendentals=0),
        compiler_params=pltpu.CompilerParams(vmem_limit_bytes=8 * 1024 * 1024),
    )(me.reshape(1).astype(jnp.int32), sphere_index.reshape(shape), table)


def finish_kernel(scale, count, order_ref, place_ref, *rest):
    out_ref, hold_ref = rest[2 * count], rest[2 * count + 1]
    length = out_ref.shape[-1]
    lefts = out_ref.shape[1]
    half = SUB // 2
    rights = 0
    for refs in (rest[:count], rest[count : 2 * count]):
        parts = []
        for part in range(refs[0].shape[1]):
            value = refs[0][0, part]
            for ref in refs[1:]:
                value = value + ref[0, part]
            parts.append(value * scale)
        if len(parts) > 1:
            real, imag, *parts = parts
            for m in range(SUB // lefts):
                rows = slice(m * lefts, (m + 1) * lefts)
                hold_ref[rights + m] = jnp.concatenate([real[rows], imag[rows]], axis=0)
            rights += SUB // lefts
        for part in parts:
            hold_ref[rights] = part
            rights += 1
    pieces = length // LANES
    for j in range(out_ref.shape[2]):
        block = hold_ref[order_ref[j]]
        for piece in range(pieces):
            lanes = slice(piece * LANES, (piece + 1) * LANES)
            place = jnp.broadcast_to(place_ref[:, lanes], (SUB, LANES))
            inner = place % LANES
            outer = place // LANES
            best = taken(block[:, :LANES], inner)
            for source in range(1, pieces):
                more = taken(block[:, source * LANES : (source + 1) * LANES], inner)
                best = jnp.where(outer == source, more, best)
            for n in range(lefts):
                out_ref[0, n, j : j + 1, lanes] = best[n : n + 1]
                out_ref[1, n, j : j + 1, lanes] = best[half + n : half + n + 1]


def finished(own, others, order, place, shape, scale):
    return pl.pallas_call(
        partial(finish_kernel, scale, len(own)),
        out_shape=jax.ShapeDtypeStruct(shape, F32),
        in_specs=[pl.BlockSpec(memory_space=pltpu.SMEM)]
        + [pl.BlockSpec(memory_space=pltpu.VMEM)] * (1 + 2 * len(own)),
        scratch_shapes=[pltpu.VMEM((shape[2], SUB, shape[-1]), F32)],
        compiler_params=pltpu.CompilerParams(vmem_limit_bytes=8 * 1024 * 1024),
    )(order, place, *own, *others)


def local(left_bands, right_bands, sphere_index, right_order):
    lefts, own_rights, planes = left_bands.shape[1], right_bands.shape[1], left_bands.shape[2]
    length, width = left_bands.shape[3], left_bands.shape[4]
    groups = lax.axis_size("grid")
    me = lax.axis_index("grid")
    per_block = sphere_index.shape[0] // groups
    slots = per_block // groups
    sizes = (groups, slots)
    cut = planes // 2
    ends = [(0, cut), (cut, planes)] if cut else [(0, planes)]
    routes = [(slice(0, own_rights - 1), 0, planes)]
    routes += [(slice(own_rights - 1, own_rights), low, high) for low, high in ends]
    sent = []
    for bands, low, high in routes:
        sent.append(swapped(right_bands[:, bands, low:high], "band", 0))

    marks = {None: 0}
    spans = []
    for bands, low, high in [(slice(0, own_rights), 0, planes)] + routes:
        pairs = lefts * (bands.stop - bands.start)
        half = low + half_planes(pairs, high - low)
        turns = []
        for plane in (low, half if half < high else low):
            turns.append(marks.setdefault(plane, len(marks)))
        spans.append((low, 0, high - low, tuple(turns)))
    offsets = tuple(marks)
    near, place, *lists = listed(
        sphere_index, me, length, width, planes, sizes, offsets
    )
    lists = (near, *lists)
    tables = (left_table(rows_table(length)), right_table(lanes_table(width)))

    def sums(right, span, before, join, last):
        return chunk_sums(left_bands, right, tables, lists, before, join, last, sizes, span)

    def owned(value):
        return grid_parts(*to_owner(value, sizes), "grid")

    early = sums(right_bands, spans[0], None, None, True)
    right, _ = lax.optimization_barrier((sent[0], early))
    early = ahead = sums(right, spans[1], None, early, True)
    final = None
    for k in range(1, len(sent)):
        right, _ = lax.optimization_barrier((sent[k], ahead))
        ahead = final = sums(right, spans[1 + k], final, None, k + 1 == len(sent))
    early = owned(early)
    final = owned(final)
    order = (right_order - lax.axis_index("band") * own_rights) % right_order.shape[0]
    shape = (2, lefts, right_order.shape[0], per_block)
    scale = 1.0 / (length * length * width) ** 0.5
    return finished(early, final, order, place, shape, scale)


def solution(mesh):
    placed = (P(None, "band", "grid", None, None), P(None, "band", "grid", None, None), P(), P())
    return jax.shard_map(
        local, mesh=mesh, in_specs=placed, out_specs=P(None, "band", None, "grid"), check_vma=False
    )
```

```python
from functools import partial
import math

import jax
import jax.numpy as jnp
import numpy as np
from jax import lax
from jax.experimental import pallas as pl
from jax.experimental.pallas import tpu as pltpu
from jax.sharding import PartitionSpec as P


F32 = jnp.float32
BF16 = jnp.bfloat16
LANES = 128
SUB = 8
VMEM_MIB = 16


def swapped(block, axis, apart):
    count = lax.axis_size(axis)
    route = []
    for low in range(count):
        high = low | 1 << apart
        if high != low and high < count:
            route += [(low, high), (high, low)]
    return lax.ppermute(block, axis, route)


def dft_parts(length):
    counter = np.arange(length)
    angles = (counter[:, None] * counter[None, :] % length) * (2.0 * math.pi / length)
    return np.cos(angles), np.sin(angles)


def two_terms(table):
    high = np.asarray(table, BF16)
    return high, np.asarray(table - np.asarray(high, np.float32), BF16)


def rows_table(length):
    cosine, sine = dft_parts(length)
    return np.block([[cosine, sine], [-sine, cosine]]).astype(np.float32)


def lanes_table(length):
    cosine, sine = dft_parts(length)
    return np.block([[cosine, -sine], [sine, cosine]]).astype(np.float32)


def left_table(table):
    high, low = two_terms(table)
    return jnp.asarray(np.concatenate([high, low, high], axis=1))


def right_table(table):
    high, low = two_terms(table)
    return jnp.asarray(np.concatenate([high, high, low], axis=0))


def split(value):
    high = value.astype(BF16)
    return high, (value - high.astype(F32)).astype(BF16)


def dot(a, b):
    return jnp.dot(a, b, preferred_element_type=F32)


def taken(value, lanes):
    return jnp.take_along_axis(value, lanes, axis=1, mode="promise_in_bounds")


def turned(number, count):
    back = 0
    while count > 1:
        back, number, count = 2 * back + number % 2, number // 2, count // 2
    return back


def window(chunk, chunks, rows):
    middle = chunk * rows // chunks
    return max(middle - 1, 0), min(middle + 2, rows)


def half_planes(pairs, planes):
    return planes // 2 if pairs < SUB and planes % 2 == 0 else planes


def chunk_kernel(
    plan, near_ref, left_ref, right_ref, table_y_ref, table_x_ref, picks_ref, places_ref, turns_ref,
    *rest,
):
    if plan["add"]:
        before_ref, *rest = rest
    if plan["join"]:
        other_kept_ref, other_sent_ref, *rest = rest
    out_ref, *rest = rest
    if plan["woven"] and plan["last"]:
        send_ref, *rest = rest
    skip = plan["join"]
    for part in range(skip):
        for spot in range(out_ref.shape[0]):
            out_ref[spot, part] = other_kept_ref[spot, part]
            send_ref[spot, part] = other_sent_ref[spot, part]
    h_real, h_imag, f_even, f_odd, hold_ref, *d_refs = rest
    lefts, rights, planes = plan["lefts"], plan["rights"], plan["planes"]
    pairs = lefts * rights
    halves, tiles, stride = plan["halves"], plan["tiles"], plan["stride"]
    length, groups, rows, chunks = plan["length"], plan["groups"], plan["rows"], plan["chunks"]
    wide = tiles * SUB
    left_low, right_low = plan["low"], plan["right_low"]

    def transform_rows(z, _):
        if halves == 2:
            slot = (z % tiles) * SUB + (z // tiles) * pairs
        else:
            slot = z * SUB
        for first in range(0, pairs, 2):
            d_ref = d_refs[first // 2]
            for k in range(2):
                m, n = (first + k) // lefts, (first + k) % lefts
                lanes = slice(k * LANES, (k + 1) * LANES)
                lr, li = left_ref[0, n, left_low + z], left_ref[1, n, left_low + z]
                rr, ri = right_ref[0, m, right_low + z], right_ref[1, m, right_low + z]
                for part, field in enumerate((lr * rr + li * ri, lr * ri - li * rr)):
                    high, low = split(field)
                    for copy, term in enumerate((high, high, low)):
                        base = (2 * copy + part) * length
                        d_ref[base : base + length, lanes] = term
            moved = dot(table_y_ref[...], d_ref[...])
            for k in range(2):
                spot = pl.ds(slot + first + k, length, stride=stride)
                lanes = slice(k * LANES, (k + 1) * LANES)
                h_real[spot, :] = moved[:length, lanes]
                h_imag[spot, :] = moved[length:, lanes]
        return 0

    def transform_two(a, _):
        transform_rows(2 * a, 0)
        return transform_rows(2 * a + 1, 0)

    if planes % 2 == 0 and pairs < SUB:
        lax.fori_loop(0, planes // 2, transform_two, 0)
    else:
        lax.fori_loop(0, planes, transform_rows, 0)

    def transform_lanes(group, f_ref):
        spots = [pl.ds((group * rows + y) * stride, wide) for y in range(rows)]
        real = jnp.concatenate([h_real[spot, :] for spot in spots], axis=0)
        imag = jnp.concatenate([h_imag[spot, :] for spot in spots], axis=0)
        high, low = split(jnp.concatenate([real, imag], axis=1))
        moved = dot(jnp.concatenate([high, low, high], axis=1), table_x_ref[...])
        for y in range(rows):
            f_ref[y] = moved[y * wide : (y + 1) * wide]

    upper = lax.broadcasted_iota(jnp.int32, (SUB, LANES), 0) >= SUB // 2
    late = lax.broadcasted_iota(jnp.int32, (SUB, LANES), 1) >= LANES // 2

    def wide_row(ref, at, *k):
        return jnp.broadcast_to(ref[k + (pl.ds(at, 1), slice(None))], (SUB, LANES))

    def box(y, tile, part):
        rows_of, lanes_of = pl.ds(tile * SUB, SUB), pl.ds(part * LANES, LANES)
        return (y, rows_of, lanes_of)

    def near(chunk, at, f_ref):
        lanes = wide_row(picks_ref, at, 0)
        start, end = window(chunk, chunks, rows)
        row_of = wide_row(picks_ref, at, 1)
        same = {y: row_of == y for y in range(start + 1, end)}

        def value(tile, part):
            best = taken(f_ref[box(start, tile, part)], lanes)
            for y in range(start + 1, end):
                best = jnp.where(same[y], taken(f_ref[box(y, tile, part)], lanes), best)
            return best

        return value

    def far(at, f_ref):
        lanes = wide_row(picks_ref, at, 0)
        y_of = wide_row(picks_ref, at, 1)

        def value(tile, part):
            def body(y, best):
                return jnp.where(y_of == y, taken(f_ref[box(y, tile, part)], lanes), best)

            return lax.fori_loop(0, rows, body, jnp.zeros((SUB, LANES), F32))

        return value

    def picked(at, value):
        first_turn, second_turn = plan["turns"]
        turn_r, turn_i = wide_row(turns_ref, at, 0, 0), wide_row(turns_ref, at, 0, 1)
        base_r = wide_row(turns_ref, at, first_turn, 0)
        base_i = wide_row(turns_ref, at, first_turn, 1)
        if halves == 2:
            base_r = jnp.where(upper, wide_row(turns_ref, at, second_turn, 0), base_r)
            base_i = jnp.where(upper, wide_row(turns_ref, at, second_turn, 1), base_i)
        real, imag = value(tiles - 1, 0), value(tiles - 1, 1)
        for tile in reversed(range(tiles - 1)):
            real, imag = (
                real * turn_r - imag * turn_i + value(tile, 0),
                real * turn_i + imag * turn_r + value(tile, 1),
            )
        real, imag = real * base_r - imag * base_i, real * base_i + imag * base_r
        if pairs == SUB:
            found = [real, imag]
        else:
            if halves == 2:
                real = real + pltpu.roll(real, SUB // 2, 0)
                imag = imag + pltpu.roll(imag, SUB // 2, 0)
            else:
                imag = pltpu.roll(imag, SUB // 2, 0)
            found = [jnp.where(upper, imag, real)]
        if plan["add"]:
            found = [one + before_ref[at, part] for part, one in enumerate(found)]
        return found

    def moved_back(group, found):
        result = []
        for chunk in range(chunks):
            place = wide_row(places_ref, group * chunks + chunk)
            lanes, source = place % LANES, place // LANES
            parts = []
            for part in range(len(found[0])):
                best = taken(found[0][part], lanes)
                for other in range(1, chunks):
                    best = jnp.where(source == other, taken(found[other][part], lanes), best)
                parts.append(best)
            result.append(parts)
        return result

    def group_sums(group, f_ref, look):
        found = []
        for chunk in range(chunks):
            at = group * chunks + chunk
            found.append(picked(at, look(chunk, at, f_ref)))
        if not plan["last"]:
            for chunk in range(chunks):
                for part, value in enumerate(found[chunk]):
                    out_ref[group * chunks + chunk, part] = value
            return found
        return moved_back(group, found)

    def put_couple(a, firsts, seconds):
        place = pl.ds(pl.multiple_of(a * LANES, LANES), LANES)
        for chunk in range(chunks):
            for part, (one, two) in enumerate(zip(firsts[chunk], seconds[chunk])):
                spot = turned(2 * chunk, groups)
                box_of = (spot, skip + part, slice(None), place)
                out_ref[box_of] = jnp.where(late, pltpu.roll(two, LANES // 2, 1), one)
                send_ref[box_of] = jnp.where(late, two, pltpu.roll(one, LANES // 2, 1))

    def put_single(group, found):
        for chunk in range(chunks):
            for part, value in enumerate(found[chunk]):
                out_ref[group * chunks + chunk, part] = value

    @pl.when(near_ref[0] == 1)
    def _():
        if groups % 2:

            def single(group, _):
                transform_lanes(group, f_even)
                found = group_sums(group, f_even, near)
                if plan["last"]:
                    put_single(group, found)
                return 0

            lax.fori_loop(0, groups, single, 0)
            return
        transform_lanes(0, f_even)

        def couple(a, _):
            transform_lanes(2 * a + 1, f_odd)
            firsts = group_sums(2 * a, f_even, near)
            transform_lanes(jnp.minimum(2 * a + 2, groups - 1), f_even)
            seconds = group_sums(2 * a + 1, f_odd, near)
            if plan["last"]:
                if plan["woven"]:
                    put_couple(a, firsts, seconds)
                else:
                    put_single(2 * a, firsts)
                    put_single(2 * a + 1, seconds)
            return 0

        def two_couples(a, _):
            couple(2 * a, 0)
            return couple(2 * a + 1, 0)

        if groups % 4 == 0 and pairs < SUB:
            lax.fori_loop(0, groups // 4, two_couples, 0)
        else:
            lax.fori_loop(0, groups // 2, couple, 0)

    @pl.when(near_ref[0] == 0)
    def _():
        def compute(group):
            transform_lanes(group, f_even)

            def body(chunk, _):
                at = group * chunks + chunk
                for part, value in enumerate(picked(at, far(at, f_even))):
                    hold_ref[chunk, part] = value
                return 0

            lax.fori_loop(0, chunks, body, 0)
            count = 2 if pairs == SUB else 1
            found = [[hold_ref[chunk, part] for part in range(count)] for chunk in range(chunks)]
            return moved_back(group, found) if plan["last"] else found

        if plan["last"] and plan["woven"]:

            def couple(a, _):
                firsts = compute(2 * a)
                put_couple(a, firsts, compute(2 * a + 1))
                return 0

            lax.fori_loop(0, groups // 2, couple, 0)
        else:

            def single(group, _):
                put_single(group, compute(group))
                return 0

            lax.fori_loop(0, groups, single, 0)


def is_woven(sizes):
    groups, slots = sizes
    return 2 * slots == LANES and groups % 2 == 0


def chunk_sums(left, right, tables, lists, before, join, last, sizes, spans):
    lefts, rights, length = left.shape[1], right.shape[1], left.shape[3]
    groups, slots = sizes
    low, right_low, planes, turns = spans
    pairs = lefts * rights
    tiles = half_planes(pairs, planes)
    wide = tiles * SUB
    stride = wide + SUB // 2
    parts = 2 * pairs // SUB
    chunks = groups * slots // LANES
    rows = length // groups
    operands = [left, right, *tables, *lists[1:]]
    if before is not None:
        operands.append(before)
    if join is not None and not is_woven(sizes):
        mine = chunk_sums(left, right, tables, lists, before, None, last, sizes, spans)
        return jnp.concatenate([join, mine], axis=1)
    if join is not None:
        operands += list(join)
    skip = 0 if join is None else join[0].shape[1]
    plan = dict(
        lefts=lefts, rights=rights, planes=planes, halves=planes // tiles, tiles=tiles,
        stride=stride, length=length, groups=groups, rows=rows, chunks=chunks,
        woven=is_woven(sizes), add=before is not None, last=last,
        low=low, right_low=right_low, turns=turns, join=skip,
    )
    if is_woven(sizes) and last:
        shape = (groups // 2, skip + parts, SUB, groups * slots)
    else:
        shape = (groups * chunks, parts, SUB, LANES)
    like = jax.ShapeDtypeStruct(shape, F32)
    field = pltpu.VMEM((length * stride, LANES), F32)
    group = pltpu.VMEM((rows, wide, 2 * LANES), F32)
    flops = 2 * 3 * 2 * pairs * planes * length * (2 * length) * (2 * length)
    return pl.pallas_call(
        partial(chunk_kernel, plan),
        out_shape=[like, like] if is_woven(sizes) and last else like,
        in_specs=[pl.BlockSpec(memory_space=pltpu.SMEM)]
        + [pl.BlockSpec(memory_space=pltpu.VMEM)] * len(operands),
        scratch_shapes=[field, field, group, group, pltpu.VMEM((chunks, parts, SUB, LANES), F32)]
        + [pltpu.VMEM((6 * length, 2 * LANES), BF16)] * (pairs // 2),
        compiler_params=pltpu.CompilerParams(vmem_limit_bytes=VMEM_MIB * 1024 * 1024),
        cost_estimate=pl.CostEstimate(flops=flops, bytes_accessed=4 * left.size, transcendentals=0),
    )(lists[0], *operands)


def to_owner(sums, sizes):
    if is_woven(sizes):
        return sums
    groups, slots = sizes
    parts = sums.shape[1]
    shaped = sums.reshape(groups, -1, parts, SUB, LANES)
    shaped = jnp.moveaxis(shaped, 1, 3).reshape(groups, parts, SUB, groups, slots)
    shaped = jnp.transpose(shaped, (3, 1, 2, 0, 4)).reshape(groups, parts, SUB, groups * slots)
    shaped = shaped[np.array([turned(owner, groups) for owner in range(groups)])]
    return shaped[: groups // 2], shaped[groups // 2 :]


def add_kernel(kept_ref, got_ref, *out_refs):
    share = kept_ref.shape[0] // len(out_refs)
    for k, out_ref in enumerate(out_refs):
        for one in range(share):
            out_ref[one] = kept_ref[k * share + one] + got_ref[k * share + one]


def added(kept, got, pieces):
    like = jax.ShapeDtypeStruct((kept.shape[0] // pieces,) + kept.shape[1:], F32)
    return pl.pallas_call(
        add_kernel,
        out_shape=[like] * pieces,
        compiler_params=pltpu.CompilerParams(vmem_limit_bytes=8 * 1024 * 1024),
    )(kept, got)


def grid_parts(kept, sent, axis):
    count = 2 * kept.shape[0]
    step = 0

    def moved(value, apart):
        route = [(device, device ^ apart) for device in range(count)]
        return lax.ppermute(value, axis, route)

    while kept.shape[0] > 4:
        got = moved(sent, 1 << step)
        kept, sent = added(kept, got, 2)
        step += 1
    got = moved(sent, 1 << step)
    kept, *sent = added(kept, got, kept.shape[0])
    low, high = 2 << step, 4 << step
    step += 1
    aparts = [high, low, low | high] if len(sent) == 3 else [low] * len(sent)
    return [kept] + [moved(one, apart) for one, apart in zip(sent, aparts)]


def over(value, count):
    if count & count - 1 == 0:
        return value >> count.bit_length() - 1
    return value // count


def rest_of(value, count):
    if count & count - 1 == 0:
        return value & count - 1
    return value % count


def list_kernel(
    plan, me_ref, index_ref, table_ref, near_ref, place_ref, picks_ref, places_ref, turns_ref, hold_ref
):
    groups, slots, rows, chunks = plan["groups"], plan["slots"], plan["rows"], plan["chunks"]
    length, width = plan["length"], plan["width"]
    size, lanes = index_ref.shape[1], index_ref.shape[0]
    total = groups * slots
    subs = total // size
    row = lax.broadcasted_iota(jnp.int32, (size, lanes), 0)
    lane = lax.broadcasted_iota(jnp.int32, (size, lanes), 1)
    spot = rest_of(lane, subs) * size + row
    flat_spot = rest_of(row, subs) * size + lane
    me = me_ref[0]

    inner_row = lax.broadcasted_iota(jnp.int32, (SUB, lanes), 0)
    sub_of = rest_of(lax.broadcasted_iota(jnp.int32, (SUB, lanes), 1), subs)

    def order_of(one, two, rising):
        small, large = jnp.minimum(one, two), jnp.maximum(one, two)
        if isinstance(rising, bool):
            return (small, large) if rising else (large, small)
        return jnp.where(rising, small, large), jnp.where(rising, large, small)

    def sort(value):
        tiles = [value[low : low + SUB] for low in range(0, size, SUB)]
        span = 2
        while span <= total:
            apart = span // 2
            while apart > 0:
                if SUB <= apart < size:
                    step = apart // SUB
                    for k in range(len(tiles)):
                        if k & step == 0:
                            if span < size:
                                rising = k * SUB & span == 0
                            elif span == total:
                                rising = True
                            else:
                                rising = sub_of & span // size == 0
                            tiles[k], tiles[k + step] = order_of(tiles[k], tiles[k + step], rising)
                else:
                    for k, tile in enumerate(tiles):
                        if apart < SUB:
                            first = inner_row & apart == 0
                            axis, shift, full = 0, apart, SUB
                        else:
                            first = sub_of & apart // size == 0
                            axis, shift, full = 1, apart // size, lanes
                        if span < SUB:
                            least = first == (inner_row & span == 0)
                        elif span < size:
                            least = first if k * SUB & span == 0 else jnp.logical_not(first)
                        elif span == total:
                            least = first
                        else:
                            least = first == (sub_of & span // size == 0)
                        other = pltpu.roll(tile, shift, axis)
                        if 2 * shift != full:
                            other = jnp.where(first, pltpu.roll(tile, full - shift, axis), other)
                        small, large = jnp.minimum(tile, other), jnp.maximum(tile, other)
                        tiles[k] = jnp.where(least, small, large)
                apart //= 2
            span *= 2
        return jnp.concatenate(tiles, axis=0)

    index = index_ref[...]
    wave_z = over(index, length * width)
    wave_y = rest_of(over(index, width), length)
    wave_x = rest_of(index, width)
    key = ((wave_y * length + wave_z) * width + wave_x) * total + flat_spot
    key = key.T
    hold_ref[...] = key.T
    mine = pltpu.roll(key, lanes - me * subs, 1)
    for sub in range(subs):
        own = jnp.broadcast_to(hold_ref[pl.ds(me * subs + sub, 1), :], (SUB, lanes))
        count = jnp.zeros((SUB, lanes), jnp.int32)
        for other in range(subs):
            column = jnp.broadcast_to(mine[:, other : other + 1], (size, lanes))
            for low in range(0, size, SUB):
                count = count + (column[low : low + SUB] < own).astype(jnp.int32)
        place_ref[:, sub * size : (sub + 1) * size] = jnp.sum(count, axis=0, keepdims=True)

    hold_ref[...] = over(sort(key), total).T
    if slots == 1:
        key = hold_ref[...]
    else:
        half = size // 2
        late = lax.broadcasted_iota(jnp.int32, (groups // 2, size), 1) >= half
        for pair in range(groups // 2):
            even = hold_ref[pl.ds(pair, groups // 2, stride=2 * subs), :]
            odd = hold_ref[pl.ds(subs + pair, groups // 2, stride=2 * subs), :]
            low = jnp.where(late, pltpu.roll(odd, half, 1), even)
            high = jnp.where(late, odd, pltpu.roll(even, half, 1))
            places_ref[pl.ds(2 * pair * subs, subs), :] = low
            places_ref[pl.ds((2 * pair + 1) * subs, subs), :] = high
        key = places_ref[...].T
    key = sort(rest_of(key, rows * length * width) * total + spot)
    hold_ref[...] = rest_of(sort(rest_of(key, total) * total + spot), total).T
    sharing = LANES // slots
    swap = lax.broadcasted_iota(jnp.int32, (groups, LANES), 1) ^ (rest_of(me, sharing) * slots)
    for chunk in range(chunks):
        other = chunk ^ over(me, sharing)
        value = hold_ref[pl.ds(other, groups, stride=chunks), :] if chunks > 1 else hold_ref[...]
        value = jnp.concatenate(
            [
                taken(value[low : low + SUB], swap[low : low + SUB])
                for low in range(0, groups, SUB)
            ],
            axis=0,
        )
        if chunks > 1:
            places_ref[pl.ds(chunk, groups, stride=chunks), :] = value
        else:
            places_ref[...] = value
    key = over(key, total).T
    row_of = over(key, width * length)
    chunk = rest_of(row, chunks)
    start, end = jnp.zeros_like(row), jnp.zeros_like(row)
    for k in range(chunks):
        lowest, above = window(k, chunks, rows)
        start, end = jnp.where(chunk == k, lowest, start), jnp.where(chunk == k, above, end)
    outside = (row_of < start) | (row_of >= end)
    near_ref[0] = 1 - jnp.max(outside.astype(F32)).astype(jnp.int32)
    picks_ref[0] = rest_of(key, width)
    picks_ref[1] = row_of
    wave_z = rest_of(over(key, width), length)
    cosine, sine = table_ref[0:1, :], table_ref[1:2, :]
    for k, offset in enumerate(plan["offsets"]):
        plane = 1 if k == 0 else me * plan["planes"] + offset
        angle = rest_of(wave_z * plane, length)
        for low in range(0, lanes, SUB):
            at = angle[low : low + SUB]
            turns_ref[k, 0, low : low + SUB] = taken(jnp.broadcast_to(cosine, (SUB, length)), at)
            turns_ref[k, 1, low : low + SUB] = taken(jnp.broadcast_to(sine, (SUB, length)), at)


def listed(sphere_index, me, length, width, planes, sizes, offsets):
    groups, slots = sizes
    total = groups * slots
    shape = (sphere_index.size // LANES, LANES)
    plan = dict(
        groups=groups, slots=slots, rows=length // groups, chunks=total // LANES, length=length,
        width=width, planes=planes, offsets=offsets,
    )
    counter = np.arange(length) * (2.0 * math.pi / length)
    table = jnp.asarray(np.stack([np.cos(counter), -np.sin(counter)]), F32)
    spec, small = pl.BlockSpec(memory_space=pltpu.VMEM), pl.BlockSpec(memory_space=pltpu.SMEM)
    whole = jax.ShapeDtypeStruct(shape, jnp.int32)
    return pl.pallas_call(
        partial(list_kernel, plan),
        out_shape=[
            jax.ShapeDtypeStruct((1,), jnp.int32),
            jax.ShapeDtypeStruct((1, total), jnp.int32),
            jax.ShapeDtypeStruct((2,) + shape, jnp.int32),
            whole,
            jax.ShapeDtypeStruct((len(offsets), 2) + shape, F32),
        ],
        in_specs=[small, spec, spec],
        out_specs=[small, spec, spec, spec, spec],
        scratch_shapes=[pltpu.VMEM(shape, jnp.int32)],
        cost_estimate=pl.CostEstimate(flops=10**10, bytes_accessed=10**6, transcendentals=0),
        compiler_params=pltpu.CompilerParams(vmem_limit_bytes=8 * 1024 * 1024),
    )(me.reshape(1).astype(jnp.int32), sphere_index.reshape(shape), table)


def finish_kernel(scale, count, order_ref, place_ref, *rest):
    out_ref, hold_ref = rest[2 * count], rest[2 * count + 1]
    length = out_ref.shape[-1]
    lefts = out_ref.shape[1]
    half = SUB // 2
    rights = 0
    for refs in (rest[:count], rest[count : 2 * count]):
        parts = []
        for part in range(refs[0].shape[1]):
            value = refs[0][0, part]
            for ref in refs[1:]:
                value = value + ref[0, part]
            parts.append(value * scale)
        if len(parts) > 1:
            real, imag, *parts = parts
            for m in range(SUB // lefts):
                rows = slice(m * lefts, (m + 1) * lefts)
                hold_ref[rights + m] = jnp.concatenate([real[rows], imag[rows]], axis=0)
            rights += SUB // lefts
        for part in parts:
            hold_ref[rights] = part
            rights += 1
    pieces = length // LANES
    for j in range(out_ref.shape[2]):
        block = hold_ref[order_ref[j]]
        for piece in range(pieces):
            lanes = slice(piece * LANES, (piece + 1) * LANES)
            place = jnp.broadcast_to(place_ref[:, lanes], (SUB, LANES))
            inner = place % LANES
            outer = place // LANES
            best = taken(block[:, :LANES], inner)
            for source in range(1, pieces):
                more = taken(block[:, source * LANES : (source + 1) * LANES], inner)
                best = jnp.where(outer == source, more, best)
            for n in range(lefts):
                out_ref[0, n, j : j + 1, lanes] = best[n : n + 1]
                out_ref[1, n, j : j + 1, lanes] = best[half + n : half + n + 1]


def finished(own, others, order, place, shape, scale):
    return pl.pallas_call(
        partial(finish_kernel, scale, len(own)),
        out_shape=jax.ShapeDtypeStruct(shape, F32),
        in_specs=[pl.BlockSpec(memory_space=pltpu.SMEM)]
        + [pl.BlockSpec(memory_space=pltpu.VMEM)] * (1 + 2 * len(own)),
        scratch_shapes=[pltpu.VMEM((shape[2], SUB, shape[-1]), F32)],
        compiler_params=pltpu.CompilerParams(vmem_limit_bytes=8 * 1024 * 1024),
    )(order, place, *own, *others)


def local(left_bands, right_bands, sphere_index, right_order):
    lefts, own_rights, planes = left_bands.shape[1], right_bands.shape[1], left_bands.shape[2]
    length, width = left_bands.shape[3], left_bands.shape[4]
    groups = lax.axis_size("grid")
    me = lax.axis_index("grid")
    per_block = sphere_index.shape[0] // groups
    slots = per_block // groups
    sizes = (groups, slots)
    cut = planes // 2
    ends = [(0, cut), (cut, planes)] if cut else [(0, planes)]
    routes = [(slice(0, own_rights - 1), 0, planes)]
    routes += [(slice(own_rights - 1, own_rights), low, high) for low, high in ends]
    sent = []
    for bands, low, high in routes:
        sent.append(swapped(right_bands[:, bands, low:high], "band", 0))

    marks = {None: 0}
    spans = []
    for bands, low, high in [(slice(0, own_rights), 0, planes)] + routes:
        pairs = lefts * (bands.stop - bands.start)
        half = low + half_planes(pairs, high - low)
        turns = []
        for plane in (low, half if half < high else low):
            turns.append(marks.setdefault(plane, len(marks)))
        spans.append((low, 0, high - low, tuple(turns)))
    offsets = tuple(marks)
    near, place, *lists = listed(
        sphere_index, me, length, width, planes, sizes, offsets
    )
    lists = (near, *lists)
    tables = (left_table(rows_table(length)), right_table(lanes_table(width)))

    def sums(right, span, before, join, last):
        return chunk_sums(left_bands, right, tables, lists, before, join, last, sizes, span)

    def owned(value):
        return grid_parts(*to_owner(value, sizes), "grid")

    early = sums(right_bands, spans[0], None, None, True)
    right, _ = lax.optimization_barrier((sent[0], early))
    early = ahead = sums(right, spans[1], None, early, True)
    final = None
    for k in range(1, len(sent)):
        right, _ = lax.optimization_barrier((sent[k], ahead))
        ahead = final = sums(right, spans[1 + k], final, None, k + 1 == len(sent))
    early = owned(early)
    final = owned(final)
    order = (right_order - lax.axis_index("band") * own_rights) % right_order.shape[0]
    shape = (2, lefts, right_order.shape[0], per_block)
    scale = 1.0 / (length * length * width) ** 0.5
    return finished(early, final, order, place, shape, scale)


def solution(mesh):
    placed = (P(None, "band", "grid", None, None), P(None, "band", "grid", None, None), P(), P())
    return jax.shard_map(
        local, mesh=mesh, in_specs=placed, out_specs=P(None, "band", None, "grid"), check_vma=False
    )
```

```python
from functools import partial
import math

import jax
import jax.numpy as jnp
import numpy as np
from jax import lax
from jax.experimental import pallas as pl
from jax.experimental.pallas import tpu as pltpu
from jax.sharding import PartitionSpec as P


F32 = jnp.float32
BF16 = jnp.bfloat16
LANES = 128
SUB = 8
VMEM_MIB = 16


def swapped(block, axis, apart):
    count = lax.axis_size(axis)
    route = []
    for low in range(count):
        high = low | 1 << apart
        if high != low and high < count:
            route += [(low, high), (high, low)]
    return lax.ppermute(block, axis, route)


def dft_parts(length):
    counter = np.arange(length)
    angles = (counter[:, None] * counter[None, :] % length) * (2.0 * math.pi / length)
    return np.cos(angles), np.sin(angles)


def two_terms(table):
    high = np.asarray(table, BF16)
    return high, np.asarray(table - np.asarray(high, np.float32), BF16)


def rows_table(length):
    cosine, sine = dft_parts(length)
    return np.block([[cosine, sine], [-sine, cosine]]).astype(np.float32)


def lanes_table(length):
    cosine, sine = dft_parts(length)
    return np.block([[cosine, -sine], [sine, cosine]]).astype(np.float32)


def left_table(table):
    high, low = two_terms(table)
    return jnp.asarray(np.concatenate([high, low, high], axis=1))


def right_table(table):
    high, low = two_terms(table)
    return jnp.asarray(np.concatenate([high, high, low], axis=0))


def split(value):
    high = value.astype(BF16)
    return high, (value - high.astype(F32)).astype(BF16)


def dot(a, b):
    return jnp.dot(a, b, preferred_element_type=F32)


def taken(value, lanes):
    return jnp.take_along_axis(value, lanes, axis=1, mode="promise_in_bounds")


def turned(number, count):
    back = 0
    while count > 1:
        back, number, count = 2 * back + number % 2, number // 2, count // 2
    return back


def window(chunk, chunks, rows):
    middle = chunk * rows // chunks
    return max(middle - 1, 0), min(middle + 2, rows)


def half_planes(pairs, planes):
    return planes // 2 if pairs < SUB and planes % 2 == 0 else planes


def chunk_kernel(
    plan, near_ref, left_ref, right_ref, table_y_ref, table_x_ref, picks_ref, places_ref, turns_ref,
    *rest,
):
    if plan["add"]:
        before_ref, *rest = rest
    if plan["join"]:
        other_kept_ref, other_sent_ref, *rest = rest
    out_ref, *rest = rest
    if plan["woven"] and plan["last"]:
        send_ref, *rest = rest
    skip = plan["join"]
    for part in range(skip):
        for spot in range(out_ref.shape[0]):
            out_ref[spot, part] = other_kept_ref[spot, part]
            send_ref[spot, part] = other_sent_ref[spot, part]
    h_real, h_imag, f_even, f_odd, hold_ref, *d_refs = rest
    lefts, rights, planes = plan["lefts"], plan["rights"], plan["planes"]
    pairs = lefts * rights
    halves, tiles, stride = plan["halves"], plan["tiles"], plan["stride"]
    length, groups, rows, chunks = plan["length"], plan["groups"], plan["rows"], plan["chunks"]
    wide = tiles * SUB
    left_low, right_low = plan["low"], plan["right_low"]

    def transform_rows(z, _):
        if halves == 2:
            slot = (z % tiles) * SUB + (z // tiles) * pairs
        else:
            slot = z * SUB
        for first in range(0, pairs, 2):
            d_ref = d_refs[first // 2]
            for k in range(2):
                m, n = (first + k) // lefts, (first + k) % lefts
                lanes = slice(k * LANES, (k + 1) * LANES)
                lr, li = left_ref[0, n, left_low + z], left_ref[1, n, left_low + z]
                rr, ri = right_ref[0, m, right_low + z], right_ref[1, m, right_low + z]
                for part, field in enumerate((lr * rr + li * ri, lr * ri - li * rr)):
                    high, low = split(field)
                    for copy, term in enumerate((high, high, low)):
                        base = (2 * copy + part) * length
                        d_ref[base : base + length, lanes] = term
            moved = dot(table_y_ref[...], d_ref[...])
            for k in range(2):
                spot = pl.ds(slot + first + k, length, stride=stride)
                lanes = slice(k * LANES, (k + 1) * LANES)
                h_real[spot, :] = moved[:length, lanes]
                h_imag[spot, :] = moved[length:, lanes]
        return 0

    def transform_two(a, _):
        transform_rows(2 * a, 0)
        return transform_rows(2 * a + 1, 0)

    if planes % 2 == 0 and pairs < SUB:
        lax.fori_loop(0, planes // 2, transform_two, 0)
    else:
        lax.fori_loop(0, planes, transform_rows, 0)

    def transform_lanes(group, f_ref):
        spots = [pl.ds((group * rows + y) * stride, wide) for y in range(rows)]
        real = jnp.concatenate([h_real[spot, :] for spot in spots], axis=0)
        imag = jnp.concatenate([h_imag[spot, :] for spot in spots], axis=0)
        high, low = split(jnp.concatenate([real, imag], axis=1))
        moved = dot(jnp.concatenate([high, low, high], axis=1), table_x_ref[...])
        for y in range(rows):
            f_ref[y] = moved[y * wide : (y + 1) * wide]

    upper = lax.broadcasted_iota(jnp.int32, (SUB, LANES), 0) >= SUB // 2
    late = lax.broadcasted_iota(jnp.int32, (SUB, LANES), 1) >= LANES // 2

    def wide_row(ref, at, *k):
        return jnp.broadcast_to(ref[k + (pl.ds(at, 1), slice(None))], (SUB, LANES))

    def box(y, tile, part):
        rows_of, lanes_of = pl.ds(tile * SUB, SUB), pl.ds(part * LANES, LANES)
        return (y, rows_of, lanes_of)

    def near(chunk, at, f_ref):
        lanes = wide_row(picks_ref, at, 0)
        start, end = window(chunk, chunks, rows)
        row_of = wide_row(picks_ref, at, 1)
        same = {y: row_of == y for y in range(start + 1, end)}

        def value(tile, part):
            best = taken(f_ref[box(start, tile, part)], lanes)
            for y in range(start + 1, end):
                best = jnp.where(same[y], taken(f_ref[box(y, tile, part)], lanes), best)
            return best

        return value

    def far(at, f_ref):
        lanes = wide_row(picks_ref, at, 0)
        y_of = wide_row(picks_ref, at, 1)

        def value(tile, part):
            def body(y, best):
                return jnp.where(y_of == y, taken(f_ref[box(y, tile, part)], lanes), best)

            return lax.fori_loop(0, rows, body, jnp.zeros((SUB, LANES), F32))

        return value

    def picked(at, value):
        first_turn, second_turn = plan["turns"]
        turn_r, turn_i = wide_row(turns_ref, at, 0, 0), wide_row(turns_ref, at, 0, 1)
        base_r = wide_row(turns_ref, at, first_turn, 0)
        base_i = wide_row(turns_ref, at, first_turn, 1)
        if halves == 2:
            base_r = jnp.where(upper, wide_row(turns_ref, at, second_turn, 0), base_r)
            base_i = jnp.where(upper, wide_row(turns_ref, at, second_turn, 1), base_i)
        real, imag = value(tiles - 1, 0), value(tiles - 1, 1)
        for tile in reversed(range(tiles - 1)):
            real, imag = (
                real * turn_r - imag * turn_i + value(tile, 0),
                real * turn_i + imag * turn_r + value(tile, 1),
            )
        real, imag = real * base_r - imag * base_i, real * base_i + imag * base_r
        if pairs == SUB:
            found = [real, imag]
        else:
            if halves == 2:
                real = real + pltpu.roll(real, SUB // 2, 0)
                imag = imag + pltpu.roll(imag, SUB // 2, 0)
            else:
                imag = pltpu.roll(imag, SUB // 2, 0)
            found = [jnp.where(upper, imag, real)]
        if plan["add"]:
            found = [one + before_ref[at, part] for part, one in enumerate(found)]
        return found

    def moved_back(group, found):
        result = []
        for chunk in range(chunks):
            place = wide_row(places_ref, group * chunks + chunk)
            lanes, source = place % LANES, place // LANES
            parts = []
            for part in range(len(found[0])):
                best = taken(found[0][part], lanes)
                for other in range(1, chunks):
                    best = jnp.where(source == other, taken(found[other][part], lanes), best)
                parts.append(best)
            result.append(parts)
        return result

    def group_sums(group, f_ref, look):
        found = []
        for chunk in range(chunks):
            at = group * chunks + chunk
            found.append(picked(at, look(chunk, at, f_ref)))
        if not plan["last"]:
            for chunk in range(chunks):
                for part, value in enumerate(found[chunk]):
                    out_ref[group * chunks + chunk, part] = value
            return found
        return moved_back(group, found)

    def put_couple(a, firsts, seconds):
        place = pl.ds(pl.multiple_of(a * LANES, LANES), LANES)
        for chunk in range(chunks):
            for part, (one, two) in enumerate(zip(firsts[chunk], seconds[chunk])):
                spot = turned(2 * chunk, groups)
                box_of = (spot, skip + part, slice(None), place)
                out_ref[box_of] = jnp.where(late, pltpu.roll(two, LANES // 2, 1), one)
                send_ref[box_of] = jnp.where(late, two, pltpu.roll(one, LANES // 2, 1))

    def put_single(group, found):
        for chunk in range(chunks):
            for part, value in enumerate(found[chunk]):
                out_ref[group * chunks + chunk, part] = value

    @pl.when(near_ref[0] == 1)
    def _():
        if groups % 2:

            def single(group, _):
                transform_lanes(group, f_even)
                found = group_sums(group, f_even, near)
                if plan["last"]:
                    put_single(group, found)
                return 0

            lax.fori_loop(0, groups, single, 0)
            return
        transform_lanes(0, f_even)

        def couple(a, _):
            transform_lanes(2 * a + 1, f_odd)
            firsts = group_sums(2 * a, f_even, near)
            transform_lanes(jnp.minimum(2 * a + 2, groups - 1), f_even)
            seconds = group_sums(2 * a + 1, f_odd, near)
            if plan["last"]:
                if plan["woven"]:
                    put_couple(a, firsts, seconds)
                else:
                    put_single(2 * a, firsts)
                    put_single(2 * a + 1, seconds)
            return 0

        batch = 4 if tiles <= 2 else 2

        def couples(a, _):
            for k in range(batch):
                couple(batch * a + k, 0)
            return 0

        if groups % (2 * batch) == 0 and pairs < SUB:
            lax.fori_loop(0, groups // (2 * batch), couples, 0)
        else:
            lax.fori_loop(0, groups // 2, couple, 0)

    @pl.when(near_ref[0] == 0)
    def _():
        def compute(group):
            transform_lanes(group, f_even)

            def body(chunk, _):
                at = group * chunks + chunk
                for part, value in enumerate(picked(at, far(at, f_even))):
                    hold_ref[chunk, part] = value
                return 0

            lax.fori_loop(0, chunks, body, 0)
            count = 2 if pairs == SUB else 1
            found = [[hold_ref[chunk, part] for part in range(count)] for chunk in range(chunks)]
            return moved_back(group, found) if plan["last"] else found

        if plan["last"] and plan["woven"]:

            def couple(a, _):
                firsts = compute(2 * a)
                put_couple(a, firsts, compute(2 * a + 1))
                return 0

            lax.fori_loop(0, groups // 2, couple, 0)
        else:

            def single(group, _):
                put_single(group, compute(group))
                return 0

            lax.fori_loop(0, groups, single, 0)


def is_woven(sizes):
    groups, slots = sizes
    return 2 * slots == LANES and groups % 2 == 0


def chunk_sums(left, right, tables, lists, before, join, last, sizes, spans):
    lefts, rights, length = left.shape[1], right.shape[1], left.shape[3]
    groups, slots = sizes
    low, right_low, planes, turns = spans
    pairs = lefts * rights
    tiles = half_planes(pairs, planes)
    wide = tiles * SUB
    stride = wide + SUB // 2
    parts = 2 * pairs // SUB
    chunks = groups * slots // LANES
    rows = length // groups
    operands = [left, right, *tables, *lists[1:]]
    if before is not None:
        operands.append(before)
    if join is not None and not is_woven(sizes):
        mine = chunk_sums(left, right, tables, lists, before, None, last, sizes, spans)
        return jnp.concatenate([join, mine], axis=1)
    if join is not None:
        operands += list(join)
    skip = 0 if join is None else join[0].shape[1]
    plan = dict(
        lefts=lefts, rights=rights, planes=planes, halves=planes // tiles, tiles=tiles,
        stride=stride, length=length, groups=groups, rows=rows, chunks=chunks,
        woven=is_woven(sizes), add=before is not None, last=last,
        low=low, right_low=right_low, turns=turns, join=skip,
    )
    if is_woven(sizes) and last:
        shape = (groups // 2, skip + parts, SUB, groups * slots)
    else:
        shape = (groups * chunks, parts, SUB, LANES)
    like = jax.ShapeDtypeStruct(shape, F32)
    field = pltpu.VMEM((length * stride, LANES), F32)
    group = pltpu.VMEM((rows, wide, 2 * LANES), F32)
    flops = 2 * 3 * 2 * pairs * planes * length * (2 * length) * (2 * length)
    return pl.pallas_call(
        partial(chunk_kernel, plan),
        out_shape=[like, like] if is_woven(sizes) and last else like,
        in_specs=[pl.BlockSpec(memory_space=pltpu.SMEM)]
        + [pl.BlockSpec(memory_space=pltpu.VMEM)] * len(operands),
        scratch_shapes=[field, field, group, group, pltpu.VMEM((chunks, parts, SUB, LANES), F32)]
        + [pltpu.VMEM((6 * length, 2 * LANES), BF16)] * (pairs // 2),
        compiler_params=pltpu.CompilerParams(vmem_limit_bytes=VMEM_MIB * 1024 * 1024),
        cost_estimate=pl.CostEstimate(flops=flops, bytes_accessed=4 * left.size, transcendentals=0),
    )(lists[0], *operands)


def to_owner(sums, sizes):
    if is_woven(sizes):
        return sums
    groups, slots = sizes
    parts = sums.shape[1]
    shaped = sums.reshape(groups, -1, parts, SUB, LANES)
    shaped = jnp.moveaxis(shaped, 1, 3).reshape(groups, parts, SUB, groups, slots)
    shaped = jnp.transpose(shaped, (3, 1, 2, 0, 4)).reshape(groups, parts, SUB, groups * slots)
    shaped = shaped[np.array([turned(owner, groups) for owner in range(groups)])]
    return shaped[: groups // 2], shaped[groups // 2 :]


def add_kernel(kept_ref, got_ref, *out_refs):
    share = kept_ref.shape[0] // len(out_refs)
    for k, out_ref in enumerate(out_refs):
        for one in range(share):
            out_ref[one] = kept_ref[k * share + one] + got_ref[k * share + one]


def added(kept, got, pieces):
    like = jax.ShapeDtypeStruct((kept.shape[0] // pieces,) + kept.shape[1:], F32)
    return pl.pallas_call(
        add_kernel,
        out_shape=[like] * pieces,
        compiler_params=pltpu.CompilerParams(vmem_limit_bytes=8 * 1024 * 1024),
    )(kept, got)


def grid_parts(kept, sent, axis):
    count = 2 * kept.shape[0]
    step = 0

    def moved(value, apart):
        route = [(device, device ^ apart) for device in range(count)]
        return lax.ppermute(value, axis, route)

    while kept.shape[0] > 4:
        got = moved(sent, 1 << step)
        kept, sent = added(kept, got, 2)
        step += 1
    got = moved(sent, 1 << step)
    kept, *sent = added(kept, got, kept.shape[0])
    low, high = 2 << step, 4 << step
    step += 1
    aparts = [high, low, low | high] if len(sent) == 3 else [low] * len(sent)
    return [kept] + [moved(one, apart) for one, apart in zip(sent, aparts)]


def over(value, count):
    if count & count - 1 == 0:
        return value >> count.bit_length() - 1
    return value // count


def rest_of(value, count):
    if count & count - 1 == 0:
        return value & count - 1
    return value % count


def list_kernel(
    plan, me_ref, index_ref, table_ref, near_ref, place_ref, picks_ref, places_ref, turns_ref, hold_ref
):
    groups, slots, rows, chunks = plan["groups"], plan["slots"], plan["rows"], plan["chunks"]
    length, width = plan["length"], plan["width"]
    size, lanes = index_ref.shape[1], index_ref.shape[0]
    total = groups * slots
    subs = total // size
    row = lax.broadcasted_iota(jnp.int32, (size, lanes), 0)
    lane = lax.broadcasted_iota(jnp.int32, (size, lanes), 1)
    spot = rest_of(lane, subs) * size + row
    flat_spot = rest_of(row, subs) * size + lane
    me = me_ref[0]

    inner_row = lax.broadcasted_iota(jnp.int32, (SUB, lanes), 0)
    sub_of = rest_of(lax.broadcasted_iota(jnp.int32, (SUB, lanes), 1), subs)

    def order_of(one, two, rising):
        small, large = jnp.minimum(one, two), jnp.maximum(one, two)
        if isinstance(rising, bool):
            return (small, large) if rising else (large, small)
        return jnp.where(rising, small, large), jnp.where(rising, large, small)

    def sort(value):
        tiles = [value[low : low + SUB] for low in range(0, size, SUB)]
        span = 2
        while span <= total:
            apart = span // 2
            while apart > 0:
                if SUB <= apart < size:
                    step = apart // SUB
                    for k in range(len(tiles)):
                        if k & step == 0:
                            if span < size:
                                rising = k * SUB & span == 0
                            elif span == total:
                                rising = True
                            else:
                                rising = sub_of & span // size == 0
                            tiles[k], tiles[k + step] = order_of(tiles[k], tiles[k + step], rising)
                else:
                    for k, tile in enumerate(tiles):
                        if apart < SUB:
                            first = inner_row & apart == 0
                            axis, shift, full = 0, apart, SUB
                        else:
                            first = sub_of & apart // size == 0
                            axis, shift, full = 1, apart // size, lanes
                        if span < SUB:
                            least = first == (inner_row & span == 0)
                        elif span < size:
                            least = first if k * SUB & span == 0 else jnp.logical_not(first)
                        elif span == total:
                            least = first
                        else:
                            least = first == (sub_of & span // size == 0)
                        other = pltpu.roll(tile, shift, axis)
                        if 2 * shift != full:
                            other = jnp.where(first, pltpu.roll(tile, full - shift, axis), other)
                        small, large = jnp.minimum(tile, other), jnp.maximum(tile, other)
                        tiles[k] = jnp.where(least, small, large)
                apart //= 2
            span *= 2
        return jnp.concatenate(tiles, axis=0)

    index = index_ref[...]
    wave_z = over(index, length * width)
    wave_y = rest_of(over(index, width), length)
    wave_x = rest_of(index, width)
    key = ((wave_y * length + wave_z) * width + wave_x) * total + flat_spot
    key = key.T
    hold_ref[...] = key.T
    mine = pltpu.roll(key, lanes - me * subs, 1)
    for sub in range(subs):
        own = jnp.broadcast_to(hold_ref[pl.ds(me * subs + sub, 1), :], (SUB, lanes))
        count = jnp.zeros((SUB, lanes), jnp.int32)
        for other in range(subs):
            column = jnp.broadcast_to(mine[:, other : other + 1], (size, lanes))
            for low in range(0, size, SUB):
                count = count + (column[low : low + SUB] < own).astype(jnp.int32)
        place_ref[:, sub * size : (sub + 1) * size] = jnp.sum(count, axis=0, keepdims=True)

    hold_ref[...] = over(sort(key), total).T
    if slots == 1:
        key = hold_ref[...]
    else:
        half = size // 2
        late = lax.broadcasted_iota(jnp.int32, (groups // 2, size), 1) >= half
        for pair in range(groups // 2):
            even = hold_ref[pl.ds(pair, groups // 2, stride=2 * subs), :]
            odd = hold_ref[pl.ds(subs + pair, groups // 2, stride=2 * subs), :]
            low = jnp.where(late, pltpu.roll(odd, half, 1), even)
            high = jnp.where(late, odd, pltpu.roll(even, half, 1))
            places_ref[pl.ds(2 * pair * subs, subs), :] = low
            places_ref[pl.ds((2 * pair + 1) * subs, subs), :] = high
        key = places_ref[...].T
    key = sort(rest_of(key, rows * length * width) * total + spot)
    hold_ref[...] = rest_of(sort(rest_of(key, total) * total + spot), total).T
    sharing = LANES // slots
    swap = lax.broadcasted_iota(jnp.int32, (groups, LANES), 1) ^ (rest_of(me, sharing) * slots)
    for chunk in range(chunks):
        other = chunk ^ over(me, sharing)
        value = hold_ref[pl.ds(other, groups, stride=chunks), :] if chunks > 1 else hold_ref[...]
        value = jnp.concatenate(
            [
                taken(value[low : low + SUB], swap[low : low + SUB])
                for low in range(0, groups, SUB)
            ],
            axis=0,
        )
        if chunks > 1:
            places_ref[pl.ds(chunk, groups, stride=chunks), :] = value
        else:
            places_ref[...] = value
    key = over(key, total).T
    row_of = over(key, width * length)
    chunk = rest_of(row, chunks)
    start, end = jnp.zeros_like(row), jnp.zeros_like(row)
    for k in range(chunks):
        lowest, above = window(k, chunks, rows)
        start, end = jnp.where(chunk == k, lowest, start), jnp.where(chunk == k, above, end)
    outside = (row_of < start) | (row_of >= end)
    near_ref[0] = 1 - jnp.max(outside.astype(F32)).astype(jnp.int32)
    picks_ref[0] = rest_of(key, width)
    picks_ref[1] = row_of
    wave_z = rest_of(over(key, width), length)
    cosine, sine = table_ref[0:1, :], table_ref[1:2, :]
    for k, offset in enumerate(plan["offsets"]):
        plane = 1 if k == 0 else me * plan["planes"] + offset
        angle = rest_of(wave_z * plane, length)
        for low in range(0, lanes, SUB):
            at = angle[low : low + SUB]
            turns_ref[k, 0, low : low + SUB] = taken(jnp.broadcast_to(cosine, (SUB, length)), at)
            turns_ref[k, 1, low : low + SUB] = taken(jnp.broadcast_to(sine, (SUB, length)), at)


def listed(sphere_index, me, length, width, planes, sizes, offsets):
    groups, slots = sizes
    total = groups * slots
    shape = (sphere_index.size // LANES, LANES)
    plan = dict(
        groups=groups, slots=slots, rows=length // groups, chunks=total // LANES, length=length,
        width=width, planes=planes, offsets=offsets,
    )
    counter = np.arange(length) * (2.0 * math.pi / length)
    table = jnp.asarray(np.stack([np.cos(counter), -np.sin(counter)]), F32)
    spec, small = pl.BlockSpec(memory_space=pltpu.VMEM), pl.BlockSpec(memory_space=pltpu.SMEM)
    whole = jax.ShapeDtypeStruct(shape, jnp.int32)
    return pl.pallas_call(
        partial(list_kernel, plan),
        out_shape=[
            jax.ShapeDtypeStruct((1,), jnp.int32),
            jax.ShapeDtypeStruct((1, total), jnp.int32),
            jax.ShapeDtypeStruct((2,) + shape, jnp.int32),
            whole,
            jax.ShapeDtypeStruct((len(offsets), 2) + shape, F32),
        ],
        in_specs=[small, spec, spec],
        out_specs=[small, spec, spec, spec, spec],
        scratch_shapes=[pltpu.VMEM(shape, jnp.int32)],
        cost_estimate=pl.CostEstimate(flops=10**10, bytes_accessed=10**6, transcendentals=0),
        compiler_params=pltpu.CompilerParams(vmem_limit_bytes=8 * 1024 * 1024),
    )(me.reshape(1).astype(jnp.int32), sphere_index.reshape(shape), table)


def finish_kernel(scale, count, order_ref, place_ref, *rest):
    out_ref, hold_ref = rest[2 * count], rest[2 * count + 1]
    length = out_ref.shape[-1]
    lefts = out_ref.shape[1]
    half = SUB // 2
    rights = 0
    for refs in (rest[:count], rest[count : 2 * count]):
        parts = []
        for part in range(refs[0].shape[1]):
            value = refs[0][0, part]
            for ref in refs[1:]:
                value = value + ref[0, part]
            parts.append(value * scale)
        if len(parts) > 1:
            real, imag, *parts = parts
            for m in range(SUB // lefts):
                rows = slice(m * lefts, (m + 1) * lefts)
                hold_ref[rights + m] = jnp.concatenate([real[rows], imag[rows]], axis=0)
            rights += SUB // lefts
        for part in parts:
            hold_ref[rights] = part
            rights += 1
    pieces = length // LANES
    for j in range(out_ref.shape[2]):
        block = hold_ref[order_ref[j]]
        for piece in range(pieces):
            lanes = slice(piece * LANES, (piece + 1) * LANES)
            place = jnp.broadcast_to(place_ref[:, lanes], (SUB, LANES))
            inner = place % LANES
            outer = place // LANES
            best = taken(block[:, :LANES], inner)
            for source in range(1, pieces):
                more = taken(block[:, source * LANES : (source + 1) * LANES], inner)
                best = jnp.where(outer == source, more, best)
            for n in range(lefts):
                out_ref[0, n, j : j + 1, lanes] = best[n : n + 1]
                out_ref[1, n, j : j + 1, lanes] = best[half + n : half + n + 1]


def finished(own, others, order, place, shape, scale):
    return pl.pallas_call(
        partial(finish_kernel, scale, len(own)),
        out_shape=jax.ShapeDtypeStruct(shape, F32),
        in_specs=[pl.BlockSpec(memory_space=pltpu.SMEM)]
        + [pl.BlockSpec(memory_space=pltpu.VMEM)] * (1 + 2 * len(own)),
        scratch_shapes=[pltpu.VMEM((shape[2], SUB, shape[-1]), F32)],
        compiler_params=pltpu.CompilerParams(vmem_limit_bytes=8 * 1024 * 1024),
    )(order, place, *own, *others)


def local(left_bands, right_bands, sphere_index, right_order):
    lefts, own_rights, planes = left_bands.shape[1], right_bands.shape[1], left_bands.shape[2]
    length, width = left_bands.shape[3], left_bands.shape[4]
    groups = lax.axis_size("grid")
    me = lax.axis_index("grid")
    per_block = sphere_index.shape[0] // groups
    slots = per_block // groups
    sizes = (groups, slots)
    cut = planes // 2
    ends = [(0, cut), (cut, planes)] if cut else [(0, planes)]
    routes = [(slice(0, own_rights - 1), 0, planes)]
    routes += [(slice(own_rights - 1, own_rights), low, high) for low, high in ends]
    sent = []
    for bands, low, high in routes:
        sent.append(swapped(right_bands[:, bands, low:high], "band", 0))

    marks = {None: 0}
    spans = []
    for bands, low, high in [(slice(0, own_rights), 0, planes)] + routes:
        pairs = lefts * (bands.stop - bands.start)
        half = low + half_planes(pairs, high - low)
        turns = []
        for plane in (low, half if half < high else low):
            turns.append(marks.setdefault(plane, len(marks)))
        spans.append((low, 0, high - low, tuple(turns)))
    offsets = tuple(marks)
    near, place, *lists = listed(
        sphere_index, me, length, width, planes, sizes, offsets
    )
    lists = (near, *lists)
    tables = (left_table(rows_table(length)), right_table(lanes_table(width)))

    def sums(right, span, before, join, last):
        return chunk_sums(left_bands, right, tables, lists, before, join, last, sizes, span)

    def owned(value):
        return grid_parts(*to_owner(value, sizes), "grid")

    early = sums(right_bands, spans[0], None, None, True)
    right, _ = lax.optimization_barrier((sent[0], early))
    early = ahead = sums(right, spans[1], None, early, True)
    final = None
    for k in range(1, len(sent)):
        right, _ = lax.optimization_barrier((sent[k], ahead))
        ahead = final = sums(right, spans[1 + k], final, None, k + 1 == len(sent))
    early = owned(early)
    final = owned(final)
    order = (right_order - lax.axis_index("band") * own_rights) % right_order.shape[0]
    shape = (2, lefts, right_order.shape[0], per_block)
    scale = 1.0 / (length * length * width) ** 0.5
    return finished(early, final, order, place, shape, scale)


def solution(mesh):
    placed = (P(None, "band", "grid", None, None), P(None, "band", "grid", None, None), P(), P())
    return jax.shard_map(
        local, mesh=mesh, in_specs=placed, out_specs=P(None, "band", None, "grid"), check_vma=False
    )
```
